256 devices in a mesh: ka: 128 (over z, y, x_hi, core), ga: 2 (over x_lo).
Axes of the slice: x: 4 (x_hi: 2, x_lo: 2; x = x_hi * 2 + x_lo), y: 4, z: 8, core: 2. Of those that a mesh axis runs over, the one named last changes fastest.
Arguments:
- coeffs: bfloat16 [128, 240, 2, 64, 128], P('ka', 'ga'), may hold values from -0.44921875 to 0.44921875
- neighbour: int32 [128, 3], P('ka'), may hold values from 0 to 127, as said below
- shift_id: int32 [128, 3], P('ka'), may hold values from 0 to 7
- block_map: int32 [8, 240], replicated, may hold values from 0 to 239, as said below
Outputs:
- intersection: float32 [128, 3, 2, 64, 64], P('ka', None, None, 'ga')
The draws below stay inside these ranges and needn't reach their ends.
Inputs may be any that keep to these rules, and one draw needn't show every extreme that they name: `neighbour`: the k-points are numbered helically. The three columns of row k hold (k + 1) mod 128, (k + 16) mod 128 and (k + 64) mod 128, in an order drawn for each row. `block_map`: each row is a permutation of the 240 blocks. Block j lies in G-slice j // 120. In every row, each G-slice receives exactly 20 of its blocks from one other G-slice, exactly 10 from each of the remaining other G-slices, and the rest from itself.
All inputs are finite; a program needn't handle non-finite values.
Results may differ from the reference program's by a relative error of at most 0.0003.
Values may be sent and summed in bfloat16 or wider, within the bound.
A program may use at most 128 MiB of HBM per device.

```python
import jax
import jax.numpy as jnp
from jax import lax

NB = 64
NBV = 3
NSHIFT = 8
K_DEV = 1
KPTS = 128
MZ = 16
NBLK = 240
BLK_SL = 120
CAP = 20
N_KA = 128
N_GA = 2


def column_order(one_key):
    return jax.random.permutation(one_key, 3).astype(jnp.int32)


def draw_neighbour(key, part):
    total = K_DEV * N_KA
    points = jnp.arange(total, dtype=jnp.int32)
    z_step = jnp.mod(points + 1, total)
    y_step = jnp.mod(points + MZ, total)
    x_step = jnp.mod(points + total // 2, total)
    stacked = jnp.stack([z_step, y_step, x_step], axis=1).astype(jnp.int32)
    orders = jax.vmap(column_order)(jax.random.split(jax.random.fold_in(key, 17), total))
    return jnp.take_along_axis(stacked, orders, axis=1).astype(jnp.int32)


def row_shuffle(one_key):
    return jax.random.permutation(one_key, BLK_SL).astype(jnp.int32)


def one_map(key):
    keys = jax.random.split(key, 3)
    lighter = CAP // 2
    heavy = jax.random.randint(keys[0], (), 1, N_GA, dtype=jnp.int32)
    rows = jnp.arange(N_GA, dtype=jnp.int32)[:, None]
    cols = jnp.arange(BLK_SL, dtype=jnp.int32)[None, :]
    self_count = BLK_SL - CAP - (N_GA - 2) * lighter
    remain = jnp.maximum(cols - self_count - CAP, 0) // lighter
    other_step = jnp.where(remain + 1 < heavy, remain + 1, remain + 2)
    offset = jnp.where(cols < self_count, 0, jnp.where(cols < self_count + CAP, heavy, other_step))
    labels = jnp.mod(rows + offset, N_GA).astype(jnp.int32)
    shuffles = jax.vmap(row_shuffle)(jax.random.split(keys[1], N_GA))
    labels = jnp.take_along_axis(labels, shuffles, axis=1).reshape(-1)
    grouped = jnp.argsort(labels, stable=True).astype(jnp.int32)
    inner = jax.vmap(row_shuffle)(jax.random.split(keys[2], N_GA))
    sources = (jnp.arange(N_GA, dtype=jnp.int32)[:, None] * BLK_SL + inner).reshape(-1)
    return jnp.zeros((N_GA * BLK_SL,), jnp.int32).at[grouped].set(sources)


def draw_block_map(key, part):
    keys = jax.random.split(key, NSHIFT)
    return jax.vmap(one_map)(keys).astype(jnp.int32)


def place_ends(values, own_key, least, top_value):
    place = [jax.random.randint(jax.random.fold_in(own_key, axis), (), 0, length) for axis, length in enumerate(values.shape)]
    main_axis = values.shape.index(max(values.shape))
    beside = place[:main_axis] + [(place[main_axis] + 1) % values.shape[main_axis]] + place[main_axis + 1:]
    return values.at[tuple(place)].set(least).at[tuple(beside)].set(top_value)


def block_scale(own_key, shape, pieces, smallest, largest):
    factor_of = 1.0
    for position, parts in pieces:
        steps = jax.random.uniform(jax.random.fold_in(jax.random.fold_in(own_key, 6), position), (parts,), jnp.float32, smallest / len(pieces), largest / len(pieces))
        factor_of = factor_of * jnp.repeat(jnp.exp(steps), shape[position] // parts).reshape((-1,) + (1,) * (len(shape) - 1 - position))
    return factor_of


def gaussian(key, extent, deviation, bound, cuts=(), held_as=jnp.bfloat16):
    loudness = block_scale(key, extent, cuts, -0.22, 0.18) if cuts else 1.0
    entries = jax.random.normal(key, extent, jnp.float32) * deviation * loudness
    return jnp.minimum(jnp.maximum(entries, -bound), bound).astype(held_as)


def setup_inputs(seed: int = 0) -> dict:
    arg_keys = jax.random.split(jax.random.key(seed), 5)
    coeffs = gaussian(arg_keys[0], (KPTS, NBLK, 2, NB, 128), 0.0755, 0.44921875, ((0, 128), (1, 2)))
    neighbour = draw_neighbour(jax.random.fold_in(arg_keys[4], 71), 0)
    shift_id = place_ends(jax.random.randint(arg_keys[2], (KPTS, NBV), 0, NSHIFT), jax.random.fold_in(arg_keys[2], 1), 0, NSHIFT - 1).astype(jnp.int32)
    block_map = draw_block_map(jax.random.fold_in(arg_keys[4], 71), 0)
    return dict(coeffs=coeffs, neighbour=neighbour, shift_id=shift_id, block_map=block_map)


def pair_product(left, right):
    return jnp.einsum("jmw,jnw->mn", left, right, precision=lax.Precision.HIGHEST)


def reference(coeffs, neighbour, shift_id, block_map):
    bra_points = (jnp.arange(KPTS * NBV, dtype=jnp.int32) // NBV).astype(jnp.int32)
    ket_points = neighbour.reshape(-1).astype(jnp.int32)
    shifts_flat = shift_id.reshape(-1).astype(jnp.int32)

    def one_pair(inputs):
        bra_point, ket_point, shift_row = inputs
        bra = coeffs[bra_point].astype(jnp.float32)
        ket = jnp.take(coeffs[ket_point], block_map[shift_row], axis=0).astype(jnp.float32)
        real_part = pair_product(bra[:, 0], ket[:, 0]) + pair_product(bra[:, 1], ket[:, 1])
        imag_part = pair_product(bra[:, 0], ket[:, 1]) - pair_product(bra[:, 1], ket[:, 0])
        return jnp.stack([real_part, imag_part])

    result = lax.map(one_pair, (bra_points, ket_points, shifts_flat))
    return result.reshape(KPTS, NBV, 2, NB, NB)
```

```python
import functools

import jax
import jax.numpy as jnp
from jax import lax
from jax.experimental import pallas as pl
from jax.experimental.pallas import tpu as pltpu
from jax.sharding import PartitionSpec as P

MESH = pl.DeviceIdType.MESH
CHUNKS = 6
STEP = 4
CONTRACT = (((1,), (1,)), ((), ()))

LOAD, ROW_SENT, RIGHT1_SENT, RIGHT1_IN, RIGHT2_SENT, RIGHT2_IN = range(6)
LEFT1_SENT, LEFT1_IN, LEFT2_SENT, LEFT2_IN, EXTRA_SENT, EXTRA_IN = range(6, 12)
RELAY_IN, RELAY_SENT, ROW_IN = range(12, 15)
ROW_JOB, NEXT_JOB, PREV_JOB, FAR_JOB, BACK_JOB = range(5)


def flipped(block):
    half = block.shape[1] // 2
    return jnp.concatenate([block[:, half:], -block[:, :half]], axis=1)


def kernel(
    n_ka, row, cross, table, coeffs, out,
    own, packed, right1, right2, left1, left2, extra, relay, ahead,
    row_out, row_in, cross_out, cross_in, parts, inbox,
    chunk_sem, row_cross_sem, cross_sem, result_sem,
):
    blocks = own.shape[0]
    bands = packed.shape[2]
    size = blocks // CHUNKS
    inside = blocks - cross
    per_job = 2 * blocks + 2 * cross
    ka = lax.axis_index("ka")
    ga = lax.axis_index("ga")
    other = 1 - ga
    core = lax.rem(ka, 2)
    plane = ka // row
    quad = lax.rem(plane, 4)
    half = plane // 4
    next_half = lax.rem(plane + 1, 8) // 4

    def at(step):
        return lax.rem(ka + n_ka + step, n_ka)

    def part(c):
        return pl.ds(c * size, size)

    def remote(source, target, sent, arrived, device):
        return pltpu.make_async_remote_copy(
            src_ref=source, dst_ref=target, send_sem=sent, recv_sem=arrived,
            device_id=device, device_id_type=MESH,
        )

    def load(c):
        return pltpu.make_async_copy(
            coeffs.at[part(c)], own.at[part(c)], chunk_sem.at[LOAD, c]
        )

    def row_direct(c):
        return remote(
            own.at[part(c)], ahead.at[part(c)],
            chunk_sem.at[ROW_SENT, c], chunk_sem.at[ROW_IN, c], (at(-1), ga),
        )

    def row_relayed(c):
        return remote(
            own.at[part(c)], relay.at[part(c)],
            chunk_sem.at[ROW_SENT, c], chunk_sem.at[RELAY_IN, c], (at(-1), other),
        )

    def relayed(c):
        return remote(
            relay.at[part(c)], ahead.at[part(c)],
            chunk_sem.at[RELAY_SENT, c], chunk_sem.at[ROW_IN, c], (ka, other),
        )

    def hop_right(c):
        return remote(
            packed.at[half, part(c)], right1.at[part(c)],
            chunk_sem.at[RIGHT1_SENT, c], chunk_sem.at[RIGHT1_IN, c], (at(row), ga),
        )

    def hop_left(c):
        return remote(
            packed.at[1 - half, part(c)], left1.at[part(c)],
            chunk_sem.at[LEFT1_SENT, c], chunk_sem.at[LEFT1_IN, c], (at(-row), ga),
        )

    def on_right(c):
        return remote(
            right1.at[part(c)], right2.at[part(c)],
            chunk_sem.at[RIGHT2_SENT, c], chunk_sem.at[RIGHT2_IN, c], (at(row), ga),
        )

    def on_left(c):
        return remote(
            left1.at[part(c)], left2.at[part(c)],
            chunk_sem.at[LEFT2_SENT, c], chunk_sem.at[LEFT2_IN, c], (at(-row), ga),
        )

    def hop_extra(c):
        return remote(
            packed.at[1 - half, part(c)], extra.at[part(c)],
            chunk_sem.at[EXTRA_SENT, c], chunk_sem.at[EXTRA_IN, c], (at(row), ga),
        )

    def swap_row():
        return remote(row_out, row_in, row_cross_sem.at[0], row_cross_sem.at[1], (ka, other))

    def swap(i):
        return remote(
            cross_out.at[i], cross_in.at[i], cross_sem.at[0, i], cross_sem.at[1, i], (ka, other)
        )

    def result(slot):
        job, step, same = RESULTS[slot]
        side = ga if same else other
        return remote(
            parts.at[job, side], inbox.at[slot],
            result_sem.at[0, slot], result_sem.at[1, slot], (at(step * row), side),
        )

    RESULTS = (
        (ROW_JOB, 0, False), (NEXT_JOB, 0, False),
        (PREV_JOB, -1, True), (PREV_JOB, -1, False),
        (FAR_JOB, -2, True), (FAR_JOB, -2, False),
        (BACK_JOB, 2, True), (BACK_JOB, 2, False),
    )

    def each(body):
        def run(c, carry):
            body(c)
            return carry
        lax.fori_loop(0, CHUNKS, run, 0)

    def bra_at(job, t):
        return table[job * per_job + t]

    def ket_at(job, t):
        return table[job * per_job + blocks + t]

    def far_ket_at(job, t):
        return table[job * per_job + 2 * blocks + cross + t]

    def gather(target, source, place):
        def run(t, carry):
            target[t] = source[place(t)]
            return carry
        lax.fori_loop(0, cross, run, 0)

    def whole_sum(total, bra, ket, count):
        def run(s, total):
            left = jnp.concatenate([bra(s * STEP + u) for u in range(STEP)], axis=1)
            right = jnp.concatenate([ket(s * STEP + u) for u in range(STEP)], axis=1)
            return total + lax.dot_general(
                left, right, CONTRACT, preferred_element_type=jnp.float32
            )
        return lax.fori_loop(0, count // STEP, run, total)

    def packed_sum(total, bra, ket, count):
        def run(s, total):
            left = jnp.concatenate([bra(s * STEP + u) for u in range(STEP)], axis=1)
            kets = [ket(s * STEP + u) for u in range(STEP)]
            right = jnp.concatenate(
                [jnp.concatenate(kets, axis=1),
                 jnp.concatenate([flipped(k) for k in kets], axis=1)], axis=0
            )
            return total + lax.dot_general(
                left, right, CONTRACT, preferred_element_type=jnp.float32
            )
        return lax.fori_loop(0, count // STEP, run, total)

    def keep(job, total):
        parts[job] = total.reshape(parts.shape[1:])

    zero = jnp.zeros((bands, 2 * bands), jnp.float32)

    each(lambda c: load(c).start())

    barrier = pltpu.get_barrier_semaphore()
    meet = [
        (ka, other), (at(row), ga), (at(-row), ga), (at(row), other), (at(-row), other),
        (at(2 * row), ga), (at(-2 * row), ga), (at(2 * row), other), (at(-2 * row), other),
        (at(-1), jnp.where(core == 1, ga, other)), (at(1), jnp.where(core == 0, ga, other)),
    ]
    for device in meet:
        pl.semaphore_signal(barrier, inc=1, device_id=device, device_id_type=MESH)
    pl.semaphore_wait(barrier, len(meet))

    def pack_chunk(c):
        def pack(t, carry):
            j = c * size + t
            real = own[j, pl.ds(0, bands), :]
            imag = own[j, pl.ds(bands, bands), :]
            cut = real.shape[1] // 2
            packed[0, j] = jnp.concatenate([real[:, :cut], imag[:, :cut]], axis=1)
            packed[1, j] = jnp.concatenate([real[:, cut:], imag[:, cut:]], axis=1)
            return carry
        lax.fori_loop(0, size, pack, 0)

    def first_sends(c):
        load(c).wait()

        @pl.when(core == 1)
        def _():
            row_direct(c).start()

        @pl.when(core == 0)
        def _():
            row_relayed(c).start()

        pack_chunk(c)

        @pl.when(c > 0)
        def _():
            hop_right(c - 1).start()
            hop_left(c - 1).start()

    each(first_sends)
    gather(row_out, own, lambda t: bra_at(ROW_JOB, inside + t))
    hop_right(CHUNKS - 1).start()
    hop_left(CHUNKS - 1).start()
    gather(cross_out.at[0], packed.at[1 - next_half], lambda t: bra_at(NEXT_JOB, inside + t))
    gather(cross_out.at[1], packed.at[half], lambda t: far_ket_at(PREV_JOB, t))
    swap_row().start()
    swap(0).start()
    swap(1).start()

    def pass_on(c):
        hop_right(c).wait_recv()
        on_right(c).start()
        hop_left(c).wait_recv()
        on_left(c).start()

        @pl.when(core == 1)
        def _():
            row_relayed(c).wait_recv()
            relayed(c).start()

    each(pass_on)

    @pl.when(quad == 3)
    def _():
        each(lambda c: hop_extra(c).start())

    swap(0).wait_recv()
    total = packed_sum(
        zero,
        lambda t: packed[1 - next_half, bra_at(NEXT_JOB, t)],
        lambda t: left1[ket_at(NEXT_JOB, t)],
        inside,
    )
    total = packed_sum(
        total, lambda t: cross_in[0, t], lambda t: left1[far_ket_at(NEXT_JOB, t)], cross
    )
    keep(NEXT_JOB, total)

    swap(1).wait_recv()

    def previous(bra):
        total = packed_sum(
            zero,
            lambda t: bra[bra_at(PREV_JOB, t)],
            lambda t: packed[half, ket_at(PREV_JOB, t)],
            inside,
        )
        total = packed_sum(
            total, lambda t: bra[bra_at(PREV_JOB, inside + t)], lambda t: cross_in[1, t], cross
        )
        keep(PREV_JOB, total)

    @pl.when(quad != 0)
    def _():
        previous(right1)

    result(1).start()

    each(lambda c: row_direct(c).wait_recv())
    swap_row().wait_recv()
    total = whole_sum(
        jnp.zeros((2 * bands, 2 * bands), jnp.float32),
        lambda t: own[bra_at(ROW_JOB, t)],
        lambda t: ahead[ket_at(ROW_JOB, t)],
        inside,
    )
    total = whole_sum(
        total, lambda t: row_in[t], lambda t: ahead[far_ket_at(ROW_JOB, t)], cross
    )
    lower = total[bands:]
    keep(
        ROW_JOB,
        total[:bands] + jnp.concatenate([lower[:, bands:], -lower[:, :bands]], axis=1),
    )

    each(lambda c: on_right(c).wait_recv())
    gather(cross_out.at[2], right2, lambda t: bra_at(FAR_JOB, inside + t))
    gather(cross_out.at[3], right2, lambda t: far_ket_at(BACK_JOB, t))
    result(0).start()
    swap(2).start()
    swap(3).start()
    each(lambda c: on_left(c).wait_recv())
    far = packed_sum(
        zero,
        lambda t: right2[bra_at(FAR_JOB, t)],
        lambda t: left2[ket_at(FAR_JOB, t)],
        inside,
    )
    back = packed_sum(
        zero,
        lambda t: left2[bra_at(BACK_JOB, t)],
        lambda t: right2[ket_at(BACK_JOB, t)],
        inside,
    )
    swap(2).wait_recv()
    far = packed_sum(
        far, lambda t: cross_in[2, t], lambda t: left2[far_ket_at(FAR_JOB, t)], cross
    )
    keep(FAR_JOB, far)
    swap(3).wait_recv()
    back = packed_sum(
        back, lambda t: left2[bra_at(BACK_JOB, inside + t)], lambda t: cross_in[3, t], cross
    )
    keep(BACK_JOB, back)

    @pl.when(quad == 0)
    def _():
        each(lambda c: hop_extra(c).wait_recv())
        previous(extra)

    for slot in (4, 5, 6, 7, 2, 3):
        result(slot).start()
    for slot in range(len(RESULTS)):
        result(slot).wait_recv()
    out[0] = parts[ROW_JOB, ga] + inbox[0]
    out[1] = (parts[NEXT_JOB, ga] + inbox[1]) + (inbox[2] + inbox[3])
    out[2] = (inbox[4] + inbox[5]) + (inbox[6] + inbox[7])

    def drain(c):
        row_direct(c).wait_send()
        hop_right(c).wait_send()
        hop_left(c).wait_send()
        on_right(c).wait_send()
        on_left(c).wait_send()

        @pl.when(core == 1)
        def _():
            relayed(c).wait_send()

        @pl.when(quad == 3)
        def _():
            hop_extra(c).wait_send()

    each(drain)
    swap_row().wait_send()
    for i in range(4):
        swap(i).wait_send()
    for slot in range(len(RESULTS)):
        result(slot).wait_send()


def job_lists(maps, my_slice, blocks, cross):
    jobs = maps.shape[0]
    source = maps.reshape(jobs, 2, blocks)
    home = jnp.arange(2, dtype=jnp.int32)[None, :, None]
    same = (source // blocks) == home
    local = lax.rem(source, blocks)
    place = jnp.arange(blocks, dtype=jnp.int32)
    before = place[None, :] < place[:, None]
    kept = jnp.sum((same[:, :, None, :] & before).astype(jnp.int32), axis=3)
    rank = jnp.where(same, kept, blocks - cross + place - kept)
    hit = rank[:, :, None, :] == place[:, None]
    bra = jnp.sum(jnp.where(hit, place, 0), axis=3)
    ket = jnp.sum(jnp.where(hit, local[:, :, None, :], 0), axis=3)
    first = my_slice == 0
    own_bra = jnp.where(first, bra[:, 0], bra[:, 1])
    own_ket = jnp.where(first, ket[:, 0], ket[:, 1])
    other_bra = jnp.where(first, bra[:, 1], bra[:, 0])[:, blocks - cross:]
    other_ket = jnp.where(first, ket[:, 1], ket[:, 0])[:, blocks - cross:]
    return jnp.concatenate([own_bra, own_ket, other_bra, other_ket], axis=1).reshape(-1)


def on_device(coeffs, neighbour, shift_id, block_map):
    _, blocks, _, bands, lanes = coeffs.shape
    n_ka = lax.axis_size("ka")
    row = n_ka // 8
    cross = 2 * max(1, blocks // 12)
    ka = lax.axis_index("ka")
    ga = lax.axis_index("ga")
    steps = jnp.array([1, row, n_ka // 2], jnp.int32)
    column = jnp.mod(ka + steps, n_ka)[:, None] == neighbour[0][None, :]
    shifts = jnp.sum(jnp.where(column, shift_id[0][None, :], 0), axis=1)

    def moved(value, step):
        return lax.ppermute(value, "ka", [(i, (i + step) % n_ka) for i in range(n_ka)])

    wanted = jnp.stack([
        shifts[0], shifts[1], moved(shifts[1], row),
        moved(shifts[2], 2 * row), moved(shifts[2], -2 * row),
    ])
    picks = wanted[:, None] == jnp.arange(block_map.shape[0], dtype=jnp.int32)[None, :]
    maps = jnp.sum(jnp.where(picks[:, :, None], block_map[None], 0), axis=1)
    table = job_lists(maps, ga, blocks, cross)

    def half_buffer(*lead):
        return pltpu.VMEM((*lead, bands, lanes), jnp.bfloat16)

    def whole_buffer(*lead):
        return pltpu.VMEM((*lead, 2 * bands, lanes), jnp.bfloat16)

    found = pl.pallas_call(
        functools.partial(kernel, n_ka, row, cross),
        out_shape=jax.ShapeDtypeStruct((3, bands // 2, 2 * bands), jnp.float32),
        in_specs=[
            pl.BlockSpec(memory_space=pltpu.SMEM),
            pl.BlockSpec(memory_space=pl.ANY),
        ],
        out_specs=pl.BlockSpec(memory_space=pltpu.VMEM),
        scratch_shapes=[
            whole_buffer(blocks),
            half_buffer(2, blocks),
            half_buffer(blocks), half_buffer(blocks),
            half_buffer(blocks), half_buffer(blocks),
            half_buffer(blocks),
            whole_buffer(blocks), whole_buffer(blocks),
            whole_buffer(cross), whole_buffer(cross),
            half_buffer(4, cross), half_buffer(4, cross),
            pltpu.VMEM((5, 2, bands // 2, 2 * bands), jnp.float32),
            pltpu.VMEM((8, bands // 2, 2 * bands), jnp.float32),
            pltpu.SemaphoreType.DMA((15, CHUNKS)),
            pltpu.SemaphoreType.DMA((2,)),
            pltpu.SemaphoreType.DMA((2, 4)),
            pltpu.SemaphoreType.DMA((2, 8)),
        ],
        compiler_params=pltpu.CompilerParams(
            collective_id=0, has_side_effects=True, vmem_limit_bytes=48 * 2**20
        ),
        name="overlaps",
    )(table, coeffs.reshape(blocks, 2 * bands, lanes))
    found = found.reshape(3, bands // 2, 2, bands).transpose(0, 2, 1, 3)
    chosen = jnp.where(
        column.T[:, :, None, None, None], found[None], jnp.zeros((), jnp.float32)
    )
    return jnp.sum(chosen, axis=1)[None]


def solution(mesh):
    in_specs = (P("ka", "ga", None, None, None), P("ka", None), P("ka", None), P())
    out_specs = P("ka", None, None, "ga", None)
    return jax.shard_map(
        on_device, mesh=mesh, in_specs=in_specs, out_specs=out_specs, check_vma=False
    )
```

```python
import functools

import jax
import jax.numpy as jnp
from jax import lax
from jax.experimental import pallas as pl
from jax.experimental.pallas import tpu as pltpu
from jax.sharding import PartitionSpec as P

MESH = pl.DeviceIdType.MESH
CHUNKS = 8
PATHS = 4
PACK = 5
STEP = 20
CONTRACT = (((1,), (1,)), ((), ()))

LOAD, ROW_SENT, RIGHT1_SENT, RIGHT1_IN, RIGHT2_SENT, RIGHT2_IN = range(6)
LEFT1_SENT, LEFT1_IN, LEFT2_SENT, LEFT2_IN = range(6, 10)
RELAY_IN, RELAY_SENT, ROW_IN = range(10, 13)
ROW_JOB, NEXT_JOB, PREV_JOB, FAR_JOB, BACK_JOB = range(5)
JOBS = 5


def flipped(block):
    half = block.shape[1] // 2
    return jnp.concatenate([block[:, half:], -block[:, :half]], axis=1)


def kernel(
    n_ka, row, cross, neighbour, shift_id, block_map, coeffs, out,
    shifts_out, shifts_in, table_rows, table, own, packed, right1, right2, left1, left2, extra, extra_out, relay, via, ahead,
    row_out, row_in, cross_out, cross_in, parts, inbox,
    chunk_sem, shift_sem, table_sem, via_sem, extra_sem, row_cross_sem, cross_sem, result_sem,
):
    blocks = own.shape[0]
    bands = packed.shape[2]
    lanes = packed.shape[3]
    size = blocks // CHUNKS
    inside = blocks - cross
    ka = lax.axis_index("ka")
    ga = lax.axis_index("ga")
    other = 1 - ga
    core = lax.rem(ka, 2)
    place = lax.rem(ka, row)
    plane = lax.rem(ka // row + 2 * core, 8)
    quad = lax.rem(plane, 4)
    half = plane // 4
    next_half = lax.rem(plane + 1, 8) // 4
    share = blocks // 2

    def at(step):
        return lax.rem(ka + n_ka + step, n_ka)

    def part(c):
        return pl.ds(c * size, size)

    def remote(source, target, sent, arrived, device):
        return pltpu.make_async_remote_copy(
            src_ref=source, dst_ref=target, send_sem=sent, recv_sem=arrived,
            device_id=device, device_id_type=MESH,
        )

    def load(c):
        return pltpu.make_async_copy(
            coeffs.at[part(c)], own.at[part(c)], chunk_sem.at[LOAD, c]
        )

    def row_direct(c):
        return remote(
            own.at[part(c)], ahead.at[part(c)],
            chunk_sem.at[ROW_SENT, c], chunk_sem.at[ROW_IN, c], (at(-1), ga),
        )

    def row_relayed(c):
        return remote(
            own.at[part(c)], relay.at[part(c)],
            chunk_sem.at[ROW_SENT, c], chunk_sem.at[RELAY_IN, c], (at(-1), other),
        )

    def relayed(c):
        return remote(
            relay.at[part(c)], ahead.at[part(c)],
            chunk_sem.at[RELAY_SENT, c], chunk_sem.at[ROW_IN, c], (ka, other),
        )

    def hop_right(c):
        return remote(
            packed.at[half, part(c)], right1.at[part(c)],
            chunk_sem.at[RIGHT1_SENT, c], chunk_sem.at[RIGHT1_IN, c], (at(row), ga),
        )

    def hop_left(c):
        return remote(
            packed.at[1 - half, part(c)], left1.at[part(c)],
            chunk_sem.at[LEFT1_SENT, c], chunk_sem.at[LEFT1_IN, c], (at(-row), ga),
        )

    def on_right(c):
        return remote(
            right1.at[part(c)], right2.at[part(c)],
            chunk_sem.at[RIGHT2_SENT, c], chunk_sem.at[RIGHT2_IN, c], (at(row), ga),
        )

    def on_left(c):
        return remote(
            left1.at[part(c)], left2.at[part(c)],
            chunk_sem.at[LEFT2_SENT, c], chunk_sem.at[LEFT2_IN, c], (at(-row), ga),
        )

    def hop_extra(step):
        return remote(
            extra_out, extra, extra_sem.at[0], extra_sem.at[1], (at(step * row), ga)
        )

    def to_via(c, p):
        slot = c // PATHS
        return remote(
            own.at[part(c)], via.at[slot],
            chunk_sem.at[ROW_SENT, c], via_sem.at[0, slot], (at(VIAS[p]), other),
        )

    def from_via(slot, p):
        c = slot * PATHS + p
        return remote(
            via.at[slot], ahead.at[part(c)],
            via_sem.at[1, slot], chunk_sem.at[ROW_IN, c], (at(-1 - VIAS[p]), other),
        )

    VIAS = {1: 2, 2: row - 4, 3: row - 2}

    def swap_row():
        return remote(row_out, row_in, row_cross_sem.at[0], row_cross_sem.at[1], (ka, other))

    def swap(i):
        return remote(
            cross_out.at[i], cross_in.at[i], cross_sem.at[0, i], cross_sem.at[1, i], (ka, other)
        )

    def result(slot):
        job, step, same = RESULTS[slot]
        side = ga if same else other
        return remote(
            parts.at[job, side], inbox.at[slot],
            result_sem.at[0, slot], result_sem.at[1, slot], (at(step * row), side),
        )

    RESULTS = (
        (ROW_JOB, 0, False), (NEXT_JOB, 0, False),
        (PREV_JOB, -1, True), (PREV_JOB, -1, False),
        (FAR_JOB, -2, True), (FAR_JOB, -2, False),
        (BACK_JOB, 2, True), (BACK_JOB, 2, False),
    )

    def each(body):
        def run(c, carry):
            body(c)
            return carry
        lax.fori_loop(0, CHUNKS, run, 0)

    def bra_at(job, t):
        return table[job, t]

    def ket_at(job, t):
        return table[JOBS + job, t]

    def far_ket_at(job, t):
        return table[2 * JOBS + job, inside + t]

    def gather(target, source, spot, count=cross):
        def run(t, carry):
            for u in range(PACK):
                target[t * PACK + u] = source[spot(t * PACK + u)]
            return carry
        lax.fori_loop(0, count // PACK, run, 0)

    def whole_sum(total, bra, ket, count):
        def run(s, total):
            left = jnp.concatenate([bra(s * STEP + u) for u in range(STEP)], axis=1)
            right = jnp.concatenate([ket(s * STEP + u) for u in range(STEP)], axis=1)
            return total + lax.dot_general(
                left, right, CONTRACT, preferred_element_type=jnp.float32
            )
        return lax.fori_loop(0, count // STEP, run, total)

    def packed_sum(total, bra, ket, count):
        def run(s, total):
            left = jnp.concatenate([bra(s * STEP + u) for u in range(STEP)], axis=1)
            kets = [ket(s * STEP + u) for u in range(STEP)]
            right = jnp.concatenate(
                [jnp.concatenate(kets, axis=1),
                 jnp.concatenate([flipped(k) for k in kets], axis=1)], axis=0
            )
            return total + lax.dot_general(
                left, right, CONTRACT, preferred_element_type=jnp.float32
            )
        return lax.fori_loop(0, count // STEP, run, total)

    def keep(job, total):
        parts[job] = total.reshape(parts.shape[1:])

    zero = jnp.zeros((bands, 2 * bands), jnp.float32)

    each(lambda c: load(c).start())

    tile = (8, lanes)
    columns = neighbour.shape[1]
    targets = [jnp.broadcast_to(neighbour[:, b : b + 1], tile) for b in range(columns)]
    steps = (1, row, n_ka // 2)

    def shift_of(step):
        found = jnp.zeros(tile, jnp.int32)
        for b in range(columns):
            moved = jnp.broadcast_to(shift_id[:, b : b + 1], tile)
            found = found + jnp.where(targets[b] == at(step), moved, 0)
        return found

    row_shift, next_shift, far_shift = [shift_of(step) for step in steps]
    shifts_out[0] = next_shift
    shifts_out[1] = far_shift

    def send_shift(i):
        return remote(
            shifts_out.at[min(i, 1)], shifts_in.at[i],
            shift_sem.at[0, i], shift_sem.at[1, i], (at((row, 2 * row, -2 * row)[i]), ga),
        )

    barrier = pltpu.get_barrier_semaphore()
    meet = [
        (ka, other), (at(row), ga), (at(-row), ga), (at(row), other), (at(-row), other),
        (at(2 * row), ga), (at(-2 * row), ga), (at(2 * row), other), (at(-2 * row), other),
        (at(-1), jnp.where(core == 1, ga, other)), (at(1), jnp.where(core == 0, ga, other)),
    ]
    for step in VIAS.values():
        meet += [(at(move), other) for move in (step, -step, 1 + step, -1 - step)]
    for device in meet:
        pl.semaphore_signal(barrier, inc=1, device_id=device, device_id_type=MESH)
    pl.semaphore_wait(barrier, len(meet))
    for i in range(3):
        send_shift(i).start()

    def pack_chunk(c):
        def pack(t, carry):
            for u in range(PACK):
                j = c * size + t * PACK + u
                real = own[j, pl.ds(0, bands), :]
                imag = own[j, pl.ds(bands, bands), :]
                cut = real.shape[1] // 2
                packed[0, j] = jnp.concatenate([real[:, :cut], imag[:, :cut]], axis=1)
                packed[1, j] = jnp.concatenate([real[:, cut:], imag[:, cut:]], axis=1)
            return carry
        lax.fori_loop(0, size // PACK, pack, 0)

    def make_table():
        lane = lax.broadcasted_iota(jnp.int32, (lanes, lanes), 1)
        line = lax.broadcasted_iota(jnp.int32, (lanes, lanes), 0)
        maps = [
            jnp.concatenate(
                [block_map[:, a * blocks : (a + 1) * blocks],
                 jnp.zeros((block_map.shape[0], lanes - blocks), jnp.int32)], axis=1
            )
            for a in range(2)
        ]
        maps = [jnp.where(ga == a, maps[0], maps[1]) for a in range(2)]
        shifts = [row_shift, next_shift] + [shifts_in[i] for i in range(3)]
        choice = lax.broadcasted_iota(jnp.int32, tile, 0)
        rows = [
            jnp.sum(jnp.where(shift == choice, each_map, 0), axis=0, keepdims=True)
            for each_map in maps for shift in shifts
        ]
        rows = jnp.concatenate(rows + [jnp.zeros((16 - 2 * JOBS, lanes), jnp.int32)], axis=0)
        number = lax.broadcasted_iota(jnp.int32, rows.shape, 0)
        spot = lax.broadcasted_iota(jnp.int32, rows.shape, 1)
        source = jnp.where(rows >= blocks, 1, 0)
        same = jnp.where(source == jnp.where(number < JOBS, ga, other), 1, 0)
        local = rows - blocks * source
        same_t = same.T
        kept = [
            jnp.sum(jnp.where(line < lane, same_t[:, r : r + 1], 0), axis=0, keepdims=True)
            for r in range(2 * JOBS)
        ]
        kept = jnp.concatenate(kept + [jnp.zeros((16 - 2 * JOBS, lanes), jnp.int32)], axis=0)
        rank = jnp.where(same == 1, kept, inside + spot - kept)
        rank_t = jnp.where(spot < blocks, rank, -1).T
        local_t = local.T
        hits = [rank_t[:, r : r + 1] == lane for r in range(2 * JOBS)]
        lists = [jnp.sum(jnp.where(hits[r], line, 0), axis=0, keepdims=True) for r in range(JOBS)]
        lists += [
            jnp.sum(jnp.where(hits[r], local_t[:, r : r + 1], 0), axis=0, keepdims=True)
            for r in range(2 * JOBS)
        ]
        lists += [jnp.zeros((1, lanes), jnp.int32)]
        table_rows[...] = jnp.concatenate(lists, axis=0)

    def first_sends(c):
        load(c).wait()

        @pl.when(core == 1)
        def _():
            row_direct(c).start()

        path = jnp.where(place == 0, lax.rem(c, PATHS), 0)

        @pl.when((core == 0) & (path == 0))
        def _():
            row_relayed(c).start()

        for p in VIAS:
            @pl.when((core == 0) & (path == p))
            def _(p=p):
                to_via(c, p).start()

        pack_chunk(c)

        @pl.when(c > 0)
        def _():
            hop_right(c - 1).start()
            hop_left(c - 1).start()

    each(first_sends)
    for i in range(3):
        send_shift(i).wait_recv()
    make_table()
    hop_right(CHUNKS - 1).start()
    hop_left(CHUNKS - 1).start()
    fetch = pltpu.make_async_copy(table_rows, table, table_sem)
    fetch.start()
    fetch.wait()
    gather(row_out, own, lambda t: bra_at(ROW_JOB, inside + t))
    gather(cross_out.at[0], packed.at[1 - next_half], lambda t: bra_at(NEXT_JOB, inside + t))
    gather(cross_out.at[1], packed.at[half], lambda t: far_ket_at(PREV_JOB, t))
    swap_row().start()
    swap(0).start()
    swap(1).start()

    def pass_on(c):
        hop_right(c).wait_recv()
        on_right(c).start()
        hop_left(c).wait_recv()
        on_left(c).start()

        @pl.when((core == 1) & (place != row - 1))
        def _():
            relay_on(c)

        for p, step in VIAS.items():
            @pl.when((place == step) & ((c == 3) | (c == 5)))
            def _(p=p):
                slot = (c - 3) // 2
                to_via(slot * PATHS, p).wait_recv()
                from_via(slot, p).start()

    def relay_on(c):
        row_relayed(c).wait_recv()
        relayed(c).start()

    each(pass_on)

    @pl.when(quad == 3)
    def _():
        gather(
            extra_out, packed.at[1 - half], lambda t: bra_at(NEXT_JOB, share + t), blocks - share
        )
        hop_extra(1).start()

    @pl.when(quad == 0)
    def _():
        gather(extra_out, packed.at[half], lambda t: ket_at(PREV_JOB, t), share)
        hop_extra(-1).start()

    @pl.when(place == row - 1)
    def _():
        for c in range(0, CHUNKS, PATHS):
            relay_on(c)

    swap(0).wait_recv()
    total = packed_sum(
        zero,
        lambda t: packed[1 - next_half, bra_at(NEXT_JOB, t)],
        lambda t: left1[ket_at(NEXT_JOB, t)],
        inside,
    )
    total = packed_sum(
        total, lambda t: cross_in[0, t], lambda t: left1[far_ket_at(NEXT_JOB, t)], cross
    )
    keep(NEXT_JOB, total)

    swap(1).wait_recv()

    @pl.when(quad != 0)
    def _():
        total = packed_sum(
            zero,
            lambda t: right1[bra_at(PREV_JOB, t)],
            lambda t: packed[half, ket_at(PREV_JOB, t)],
            inside,
        )
        total = packed_sum(
            total, lambda t: right1[bra_at(PREV_JOB, inside + t)], lambda t: cross_in[1, t], cross
        )
        keep(PREV_JOB, total)

    @pl.when(quad != 3)
    def _():
        result(1).start()

    each(lambda c: row_direct(c).wait_recv())
    swap_row().wait_recv()
    total = whole_sum(
        jnp.zeros((2 * bands, 2 * bands), jnp.float32),
        lambda t: own[bra_at(ROW_JOB, t)],
        lambda t: ahead[ket_at(ROW_JOB, t)],
        inside,
    )
    total = whole_sum(
        total, lambda t: row_in[t], lambda t: ahead[far_ket_at(ROW_JOB, t)], cross
    )
    lower = total[bands:]
    keep(
        ROW_JOB,
        total[:bands] + jnp.concatenate([lower[:, bands:], -lower[:, :bands]], axis=1),
    )

    each(lambda c: on_right(c).wait_recv())
    gather(cross_out.at[2], right2, lambda t: bra_at(FAR_JOB, inside + t))
    gather(cross_out.at[3], right2, lambda t: far_ket_at(BACK_JOB, t))
    result(0).start()

    @pl.when(quad != 0)
    def _():
        result(2).start()
        result(3).start()

    swap(2).start()
    swap(3).start()
    each(lambda c: on_left(c).wait_recv())
    far = packed_sum(
        zero,
        lambda t: right2[bra_at(FAR_JOB, t)],
        lambda t: left2[ket_at(FAR_JOB, t)],
        inside,
    )
    back = packed_sum(
        zero,
        lambda t: left2[bra_at(BACK_JOB, t)],
        lambda t: right2[ket_at(BACK_JOB, t)],
        inside,
    )
    swap(2).wait_recv()
    far = packed_sum(
        far, lambda t: cross_in[2, t], lambda t: left2[far_ket_at(FAR_JOB, t)], cross
    )
    keep(FAR_JOB, far)
    swap(3).wait_recv()
    back = packed_sum(
        back, lambda t: left2[bra_at(BACK_JOB, inside + t)], lambda t: cross_in[3, t], cross
    )
    keep(BACK_JOB, back)

    for slot in (4, 5, 6, 7):
        result(slot).start()

    @pl.when(quad == 3)
    def _():
        hop_extra(1).wait_recv()
        more = packed_sum(
            zero,
            lambda t: packed[1 - half, bra_at(NEXT_JOB, t)],
            lambda t: extra[t],
            share,
        )
        keep(NEXT_JOB, parts[NEXT_JOB].reshape(zero.shape) + more)
        result(1).start()

    @pl.when(quad == 0)
    def _():
        hop_extra(-1).wait_recv()
        total = packed_sum(
            zero,
            lambda t: extra[t],
            lambda t: packed[half, ket_at(PREV_JOB, share + t)],
            inside - share,
        )
        total = packed_sum(
            total, lambda t: extra[inside - share + t], lambda t: cross_in[1, t], cross
        )
        keep(PREV_JOB, total)
        result(2).start()
        result(3).start()
    for slot in range(len(RESULTS)):
        result(slot).wait_recv()
    found = [
        parts[ROW_JOB, ga] + inbox[0],
        (parts[NEXT_JOB, ga] + inbox[1]) + (inbox[2] + inbox[3]),
        (inbox[4] + inbox[5]) + (inbox[6] + inbox[7]),
    ]
    for b in range(columns):
        target = jnp.broadcast_to(neighbour[:, b : b + 1], found[0].shape)
        chosen = jnp.where(
            target == at(steps[0]), found[0], jnp.where(target == at(steps[1]), found[1], found[2])
        )
        out[b, 0] = chosen[:, :bands]
        out[b, 1] = chosen[:, bands:]

    def drain(c):
        row_direct(c).wait_send()
        hop_right(c).wait_send()
        hop_left(c).wait_send()
        on_right(c).wait_send()
        on_left(c).wait_send()

        @pl.when((core == 1) & ((place != row - 1) | (lax.rem(c, PATHS) == 0)))
        def _():
            relayed(c).wait_send()

    each(drain)
    for i in range(3):
        send_shift(i).wait_send()

    @pl.when((quad == 3) | (quad == 0))
    def _():
        hop_extra(1).wait_send()

    for p, step in VIAS.items():
        @pl.when(place == step)
        def _(p=p):
            for slot in range(CHUNKS // PATHS):
                from_via(slot, p).wait_send()

    swap_row().wait_send()
    for i in range(4):
        swap(i).wait_send()
    for slot in range(len(RESULTS)):
        result(slot).wait_send()


def on_device(coeffs, neighbour, shift_id, block_map):
    _, blocks, _, bands, lanes = coeffs.shape
    columns = neighbour.shape[1]
    n_ka = lax.axis_size("ka")
    row = n_ka // 8
    cross = 2 * max(1, blocks // 12)
    def half_buffer(*lead):
        return pltpu.VMEM((*lead, bands, lanes), jnp.bfloat16)

    def whole_buffer(*lead):
        return pltpu.VMEM((*lead, 2 * bands, lanes), jnp.bfloat16)

    found = pl.pallas_call(
        functools.partial(kernel, n_ka, row, cross),
        out_shape=jax.ShapeDtypeStruct((columns, 2, bands // 2, bands), jnp.float32),
        in_specs=[
            pl.BlockSpec(memory_space=pltpu.VMEM),
            pl.BlockSpec(memory_space=pltpu.VMEM),
            pl.BlockSpec(memory_space=pltpu.VMEM),
            pl.BlockSpec(memory_space=pl.ANY),
        ],
        out_specs=pl.BlockSpec(memory_space=pltpu.VMEM),
        scratch_shapes=[
            pltpu.VMEM((2, 8, lanes), jnp.int32),
            pltpu.VMEM((3, 8, lanes), jnp.int32),
            pltpu.VMEM((16, lanes), jnp.int32),
            pltpu.SMEM((16, lanes), jnp.int32),
            whole_buffer(blocks),
            half_buffer(2, blocks),
            half_buffer(blocks), half_buffer(blocks),
            half_buffer(blocks), half_buffer(blocks),
            half_buffer(blocks // 2), half_buffer(blocks // 2),
            whole_buffer(blocks), whole_buffer(CHUNKS // PATHS, blocks // CHUNKS),
            whole_buffer(blocks),
            whole_buffer(cross), whole_buffer(cross),
            half_buffer(4, cross), half_buffer(4, cross),
            pltpu.VMEM((5, 2, bands // 2, 2 * bands), jnp.float32),
            pltpu.VMEM((8, bands // 2, 2 * bands), jnp.float32),
            pltpu.SemaphoreType.DMA((13, CHUNKS)),
            pltpu.SemaphoreType.DMA((2, 3)),
            pltpu.SemaphoreType.DMA,
            pltpu.SemaphoreType.DMA((2, CHUNKS // PATHS)),
            pltpu.SemaphoreType.DMA((2,)),
            pltpu.SemaphoreType.DMA((2,)),
            pltpu.SemaphoreType.DMA((2, 4)),
            pltpu.SemaphoreType.DMA((2, 8)),
        ],
        compiler_params=pltpu.CompilerParams(
            collective_id=0, has_side_effects=True, vmem_limit_bytes=61 * 2**20
        ),
        name="overlaps",
    )(neighbour, shift_id, block_map, coeffs.reshape(blocks, 2 * bands, lanes))
    return found[None]


def solution(mesh):
    in_specs = (P("ka", "ga", None, None, None), P("ka", None), P("ka", None), P())
    out_specs = P("ka", None, None, "ga", None)
    return jax.shard_map(
        on_device, mesh=mesh, in_specs=in_specs, out_specs=out_specs, check_vma=False
    )
```

```python
import functools

import jax
import jax.numpy as jnp
from jax import lax
from jax.experimental import pallas as pl
from jax.experimental.pallas import tpu as pltpu
from jax.sharding import PartitionSpec as P

MESH = pl.DeviceIdType.MESH
CHUNKS = 8
CUTS = 4
TURNS = 6
LEFT_OWN, LEFT_BESIDE = (0,), (1,)
RIGHT_OWN, RIGHT_BESIDE = (2, 3), (4, 5)
LEFT = LEFT_OWN + LEFT_BESIDE
RIGHT = RIGHT_OWN + RIGHT_BESIDE
PACK = 5
STEP = 20
CONTRACT = (((1,), (1,)), ((), ()))

LOAD, ROW_SENT, RELAY_IN, RELAY_SENT, ROW_IN = range(5)
RIGHT1_SENT, RIGHT1_IN, RIGHT2_SENT, RIGHT2_IN = range(4)
LEFT1_SENT, LEFT1_IN, LEFT2_SENT, LEFT2_IN = range(4, 8)
ROW_JOB, NEXT_JOB, PREV_JOB, FAR_JOB, BACK_JOB = range(5)
JOBS = 5


def flipped(block):
    half = block.shape[1] // 2
    return jnp.concatenate([block[:, half:], -block[:, :half]], axis=1)


def kernel(
    n_ka, row, cross, neighbour, shift_id, block_map, coeffs, out,
    shifts_out, shifts_in, table_rows, table, own, packed, right1, right2_0, right2_1, right2_2, right2_3, left1, left2,
    extra, extra_out, extra_via, relay, via, ahead,
    row_out, row_in, cross_out, cross_in, far_out, far_in, row_total, parts, inbox,
    chunk_sem, hop_sem, shift_sem, table_sem, via_sem, extra_sem, row_cross_sem, cross_sem,
    far_sem, result_sem,
):
    blocks = own.shape[0]
    bands = own.shape[1] // 2
    lanes = own.shape[2]
    deep = bands // CUTS
    right2 = (right2_0, right2_1, right2_2, right2_3)
    size = blocks // CHUNKS
    inside = blocks - cross
    ka = lax.axis_index("ka")
    ga = lax.axis_index("ga")
    other = 1 - ga
    core = lax.rem(ka, 2)
    place = lax.rem(ka, row)
    odd = lax.rem(place // 4, 2)
    aside = 4 - 8 * odd
    plane = lax.rem(ka // row + 2 * core + odd, 8)
    beside = lax.rem(ka // row + 2 * core + 1 - odd, 4)
    quad = lax.rem(plane, 4)
    half = plane // 4
    needs_row = (core == 0) | (place == row - 1)
    next_half = lax.rem(plane + 1, 8) // 4

    def at(step):
        return lax.rem(ka + n_ka + step, n_ka)

    def part(c):
        return pl.ds(c * size, size)

    def remote(source, target, sent, arrived, device):
        return pltpu.make_async_remote_copy(
            src_ref=source, dst_ref=target, send_sem=sent, recv_sem=arrived,
            device_id=device, device_id_type=MESH,
        )

    def load(c):
        return pltpu.make_async_copy(
            coeffs.at[part(c)], own.at[part(c)], chunk_sem.at[LOAD, c]
        )

    def row_direct(c):
        return remote(
            own.at[part(c)], ahead.at[part(c)],
            chunk_sem.at[ROW_SENT, c], chunk_sem.at[ROW_IN, c], (at(-1), ga),
        )

    def row_relayed(c):
        return remote(
            own.at[part(c)], relay.at[part(c)],
            chunk_sem.at[ROW_SENT, c], chunk_sem.at[RELAY_IN, c], (at(-1), other),
        )

    def relayed(c):
        return remote(
            relay.at[part(c)], ahead.at[part(c)],
            chunk_sem.at[RELAY_SENT, c], chunk_sem.at[ROW_IN, c], (ka, other),
        )

    def hop(source, target, sent, cut, step):
        return remote(
            source, target, hop_sem.at[sent, cut], hop_sem.at[sent + 1, cut], (at(step * row), ga)
        )

    def hop_right(cut):
        return hop(packed.at[half, cut], right1.at[cut], RIGHT1_SENT, cut, 1)

    def hop_left(cut):
        return hop(packed.at[1 - half, cut], left1.at[cut], LEFT1_SENT, cut, -1)

    def on_right(cut):
        return hop(right1.at[cut], right2[cut], RIGHT2_SENT, cut, 1)

    def on_left(cut):
        return hop(left1.at[cut], left2.at[cut], LEFT2_SENT, cut, -1)

    def hop_extra(turn):
        step = -1 if turn in LEFT else 1
        return remote(
            extra_out.at[turn], extra.at[turn],
            extra_sem.at[0, turn], extra_sem.at[1, turn], (at(step * row), ga),
        )

    def extra_aside(turn):
        return remote(
            extra_out.at[turn], extra_via.at[turn],
            extra_sem.at[0, turn], extra_sem.at[2, turn], (at(aside), ga),
        )

    def extra_back(turn):
        step = -1 if turn in LEFT else 1
        return remote(
            extra_via.at[turn], extra.at[turn],
            extra_sem.at[3, turn], extra_sem.at[1, turn], (at(aside + step * row), ga),
        )

    def to_via(c):
        return remote(
            own.at[part(c)], via, chunk_sem.at[ROW_SENT, c], via_sem.at[0], (at(2 * c), other)
        )

    def from_via():
        c = place // 2
        return remote(
            via, ahead.at[part(c)], via_sem.at[1], chunk_sem.at[ROW_IN, c],
            (at(-1 - place), other),
        )

    def swap_row():
        return remote(row_out, row_in, row_cross_sem.at[0], row_cross_sem.at[1], (ka, other))

    def swap(i):
        return remote(
            cross_out.at[i], cross_in.at[i], cross_sem.at[0, i], cross_sem.at[1, i], (ka, other)
        )

    def swap_far(i, cut):
        return remote(
            far_out.at[i, cut], far_in.at[i, cut],
            far_sem.at[0, i, cut], far_sem.at[1, i, cut], (ka, other),
        )

    def result(slot):
        job, step, same = RESULTS[slot]
        side = ga if same else other
        return remote(
            parts.at[job, side], inbox.at[slot],
            result_sem.at[0, slot], result_sem.at[1, slot], (at(step * row), side),
        )

    RESULTS = (
        (ROW_JOB, 0, False), (NEXT_JOB, 0, False),
        (PREV_JOB, -1, True), (PREV_JOB, -1, False),
        (FAR_JOB, -2, True), (FAR_JOB, -2, False),
        (BACK_JOB, 2, True), (BACK_JOB, 2, False),
    )

    def each(body):
        def run(c, carry):
            body(c)
            return carry
        lax.fori_loop(0, CHUNKS, run, 0)

    def bra_at(job, t):
        return table[job, t]

    def ket_at(job, t):
        return table[JOBS + job, t]

    def far_ket_at(job, t):
        return table[2 * JOBS + job, inside + t]

    def whole(source, index):
        return jnp.concatenate([source[cut, index] for cut in range(CUTS)], axis=0)

    def whole_far(index):
        return jnp.concatenate([right2[cut][index] for cut in range(CUTS)], axis=0)

    def gather(target, pick):
        def run(t, carry):
            for u in range(PACK):
                target[t * PACK + u] = pick(t * PACK + u)
            return carry
        lax.fori_loop(0, cross // PACK, run, 0)

    def whole_sum(total, bra, ket, count):
        def run(s, total):
            left = jnp.concatenate([bra(s * STEP + u) for u in range(STEP)], axis=1)
            right = jnp.concatenate([ket(s * STEP + u) for u in range(STEP)], axis=1)
            return total + lax.dot_general(
                left, right, CONTRACT, preferred_element_type=jnp.float32
            )
        return lax.fori_loop(0, count // STEP, run, total)

    def packed_sum(total, bra, ket, count):
        def run(s, total):
            left = jnp.concatenate([bra(s * STEP + u) for u in range(STEP)], axis=1)
            kets = [ket(s * STEP + u) for u in range(STEP)]
            right = jnp.concatenate(
                [jnp.concatenate(kets, axis=1),
                 jnp.concatenate([flipped(k) for k in kets], axis=1)], axis=0
            )
            return total + lax.dot_general(
                left, right, CONTRACT, preferred_element_type=jnp.float32
            )
        return lax.fori_loop(0, count // STEP, run, total)

    def keep(job, total):
        parts[job] = total.reshape(parts.shape[1:])

    zero = jnp.zeros((bands, 2 * bands), jnp.float32)

    each(lambda c: load(c).start())

    tile = (8, lanes)
    columns = neighbour.shape[1]
    targets = [jnp.broadcast_to(neighbour[:, b : b + 1], tile) for b in range(columns)]
    steps = (1, row, n_ka // 2)

    def shift_of(step):
        found = jnp.zeros(tile, jnp.int32)
        for b in range(columns):
            moved = jnp.broadcast_to(shift_id[:, b : b + 1], tile)
            found = found + jnp.where(targets[b] == at(step), moved, 0)
        return found

    row_shift, next_shift, far_shift = [shift_of(step) for step in steps]
    shifts_out[0] = next_shift
    shifts_out[1] = far_shift

    def send_shift(i):
        return remote(
            shifts_out.at[min(i, 1)], shifts_in.at[i],
            shift_sem.at[0, i], shift_sem.at[1, i], (at((row, 2 * row, -2 * row)[i]), ga),
        )

    barrier = pltpu.get_barrier_semaphore()
    meet = [
        (ka, other), (at(row), ga), (at(-row), ga), (at(row), other), (at(-row), other),
        (at(2 * row), ga), (at(-2 * row), ga), (at(2 * row), other), (at(-2 * row), other),
        (at(-1), jnp.where(core == 1, ga, other)), (at(1), jnp.where(core == 0, ga, other)),
        (at(aside), ga), (at(aside + row), ga), (at(aside - row), ga),
    ]
    paths = row // 2

    def greet(device):
        pl.semaphore_signal(barrier, inc=1, device_id=device, device_id_type=MESH)

    for device in meet:
        greet(device)

    @pl.when(place == 0)
    def _():
        for p in range(1, paths):
            greet((at(2 * p), other))

    @pl.when(place == row - 1)
    def _():
        for p in range(1, paths):
            greet((at(1 + 2 * p), other))

    between = (core == 0) & (place > 0)

    @pl.when(between)
    def _():
        greet((at(-place), other))
        greet((at(-1 - place), other))

    def pack_cut(cut):
        def pack(t, carry):
            for u in range(STEP):
                j = t * STEP + u
                real = own[j, pl.ds(cut * deep, deep), :]
                imag = own[j, pl.ds(bands + cut * deep, deep), :]
                mid = lanes // 2
                packed[0, cut, j] = jnp.concatenate([real[:, :mid], imag[:, :mid]], axis=1)
                packed[1, cut, j] = jnp.concatenate([real[:, mid:], imag[:, mid:]], axis=1)
            return carry
        lax.fori_loop(0, blocks // STEP, pack, 0)

    each(lambda c: load(c).wait())
    pack_cut(0)
    ends = (place == 0) | (place == row - 1)
    pl.semaphore_wait(
        barrier, len(meet) + jnp.where(ends, paths - 1, 0) + jnp.where(between, 2, 0)
    )
    for i in range(3):
        send_shift(i).start()

    def make_table():
        lane = lax.broadcasted_iota(jnp.int32, (lanes, lanes), 1)
        line = lax.broadcasted_iota(jnp.int32, (lanes, lanes), 0)
        maps = [
            jnp.concatenate(
                [block_map[:, a * blocks : (a + 1) * blocks],
                 jnp.zeros((block_map.shape[0], lanes - blocks), jnp.int32)], axis=1
            )
            for a in range(2)
        ]
        maps = [jnp.where(ga == a, maps[0], maps[1]) for a in range(2)]
        shifts = [row_shift, next_shift] + [shifts_in[i] for i in range(3)]
        choice = lax.broadcasted_iota(jnp.int32, tile, 0)
        rows = [
            jnp.sum(jnp.where(shift == choice, each_map, 0), axis=0, keepdims=True)
            for each_map in maps for shift in shifts
        ]
        rows = jnp.concatenate(rows + [jnp.zeros((16 - 2 * JOBS, lanes), jnp.int32)], axis=0)
        number = lax.broadcasted_iota(jnp.int32, rows.shape, 0)
        spot = lax.broadcasted_iota(jnp.int32, rows.shape, 1)
        source = jnp.where(rows >= blocks, 1, 0)
        same = jnp.where(source == jnp.where(number < JOBS, ga, other), 1, 0)
        local = rows - blocks * source
        same_t = same.T
        kept = [
            jnp.sum(jnp.where(line < lane, same_t[:, r : r + 1], 0), axis=0, keepdims=True)
            for r in range(2 * JOBS)
        ]
        kept = jnp.concatenate(kept + [jnp.zeros((16 - 2 * JOBS, lanes), jnp.int32)], axis=0)
        rank = jnp.where(same == 1, kept, inside + spot - kept)
        rank_t = jnp.where(spot < blocks, rank, -1).T
        local_t = local.T
        hits = [rank_t[:, r : r + 1] == lane for r in range(2 * JOBS)]
        lists = [jnp.sum(jnp.where(hits[r], line, 0), axis=0, keepdims=True) for r in range(JOBS)]
        lists += [
            jnp.sum(jnp.where(hits[r], local_t[:, r : r + 1], 0), axis=0, keepdims=True)
            for r in range(2 * JOBS)
        ]
        lists += [jnp.zeros((1, lanes), jnp.int32)]
        table_rows[...] = jnp.concatenate(lists, axis=0)

    def first_sends(c):
        @pl.when(core == 1)
        def _():
            row_direct(c).start()

        @pl.when((core == 0) & ((place > 0) | (c == 0)))
        def _():
            row_relayed(c).start()

        @pl.when((place == 0) & (c > 0))
        def _():
            to_via(c).start()

    each(first_sends)
    hop_right(0).start()
    hop_left(0).start()
    pack_cut(1)
    for cut in range(1, CUTS):
        if cut + 1 < CUTS:
            pack_cut(cut + 1)
        hop_right(cut).start()
        hop_left(cut).start()
    for i in range(3):
        send_shift(i).wait_recv()
    make_table()
    fetch = pltpu.make_async_copy(table_rows, table, table_sem)
    fetch.start()
    fetch.wait()
    gather(cross_out.at[0], lambda t: whole(packed.at[1 - next_half], bra_at(NEXT_JOB, inside + t)))
    gather(cross_out.at[1], lambda t: whole(packed.at[half], far_ket_at(PREV_JOB, t)))

    @pl.when(needs_row)
    def _():
        gather(row_out, lambda t: own[bra_at(ROW_JOB, inside + t)])
        swap_row().start()

    swap(0).start()
    swap(1).start()

    @pl.when(quad == 3)
    def _():
        for turn in RIGHT_BESIDE + RIGHT_OWN:
            gather(
                extra_out.at[turn],
                lambda t: whole(packed.at[1 - half], bra_at(NEXT_JOB, turn * cross + t)),
            )
        for turn in RIGHT_BESIDE:
            extra_aside(turn).start()

    @pl.when(quad == 0)
    def _():
        for turn in LEFT_BESIDE + LEFT_OWN:
            gather(
                extra_out.at[turn],
                lambda t: whole(packed.at[half], ket_at(PREV_JOB, turn * cross + t)),
            )
        for turn in LEFT_BESIDE:
            extra_aside(turn).start()

    def relay_on(c):
        row_relayed(c).wait_recv()
        relayed(c).start()

    for cut in range(CUTS):
        hop_right(cut).wait_recv()
        on_right(cut).start()
        hop_left(cut).wait_recv()

        @pl.when(between & ((place - 2) // 4 == cut))
        def _():
            to_via(0).wait_recv()
            from_via().start()

        on_left(cut).start()

        @pl.when((core == 1) & (place < row - 1))
        def _(cut=cut):
            for c in range(cut * CHUNKS // CUTS, (cut + 1) * CHUNKS // CUTS):
                relay_on(c)

        if cut == 1:
            @pl.when(place == row - 1)
            def _():
                relay_on(0)

    @pl.when(quad == 3)
    def _():
        for turn in RIGHT_OWN:
            hop_extra(turn).start()

    @pl.when(quad == 0)
    def _():
        for turn in LEFT_OWN:
            hop_extra(turn).start()

    @pl.when(beside == 3)
    def _():
        for turn in RIGHT_BESIDE:
            extra_aside(turn).wait_recv()
            extra_back(turn).start()

    @pl.when(beside == 0)
    def _():
        for turn in LEFT_BESIDE:
            extra_aside(turn).wait_recv()
            extra_back(turn).start()

    swap(0).wait_recv()
    total = packed_sum(
        zero,
        lambda t: whole(packed.at[1 - next_half], bra_at(NEXT_JOB, t)),
        lambda t: whole(left1, ket_at(NEXT_JOB, t)),
        inside,
    )
    total = packed_sum(
        total, lambda t: cross_in[0, t], lambda t: whole(left1, far_ket_at(NEXT_JOB, t)), cross
    )
    keep(NEXT_JOB, total)

    swap(1).wait_recv()

    @pl.when(quad != 0)
    def _():
        total = packed_sum(
            zero,
            lambda t: whole(right1, bra_at(PREV_JOB, t)),
            lambda t: whole(packed.at[half], ket_at(PREV_JOB, t)),
            inside,
        )
        total = packed_sum(
            total,
            lambda t: whole(right1, bra_at(PREV_JOB, inside + t)),
            lambda t: cross_in[1, t],
            cross,
        )
        keep(PREV_JOB, total)

    @pl.when(quad != 3)
    def _():
        result(1).start()

    def along_row():
        each(lambda c: row_direct(c).wait_recv())
        row_total[...] = whole_sum(
            jnp.zeros(row_total.shape, jnp.float32),
            lambda t: own[bra_at(ROW_JOB, t)],
            lambda t: ahead[ket_at(ROW_JOB, t)],
            inside,
        )

        @pl.when(needs_row)
        def _():
            swap_row().wait_recv()
            row_total[...] = whole_sum(
                row_total[...], lambda t: row_in[t], lambda t: ahead[far_ket_at(ROW_JOB, t)], cross
            )

        @pl.when(jnp.logical_not(needs_row))
        def _():
            row_total[...] = whole_sum(
                row_total[...],
                lambda t: own[bra_at(ROW_JOB, inside + t)],
                lambda t: relay[ket_at(ROW_JOB, inside + t)],
                cross,
            )

        lower = row_total[pl.ds(bands, bands)]
        keep(
            ROW_JOB,
            row_total[pl.ds(0, bands)]
            + jnp.concatenate([lower[:, bands:], -lower[:, :bands]], axis=1),
        )
        result(0).start()

    @pl.when(core == 0)
    def _():
        along_row()

    def far_swaps(cut):
        on_right(cut).wait_recv()
        gather(far_out.at[0, cut], lambda t: right2[cut][bra_at(FAR_JOB, inside + t)])
        gather(far_out.at[1, cut], lambda t: right2[cut][far_ket_at(BACK_JOB, t)])
        swap_far(0, cut).start()
        swap_far(1, cut).start()

    far_swaps(0)

    @pl.when(quad != 0)
    def _():
        result(2).start()
        result(3).start()

    for cut in range(1, CUTS):
        far_swaps(cut)

    for cut in range(CUTS):
        on_left(cut).wait_recv()
    far = packed_sum(
        zero,
        lambda t: whole_far(bra_at(FAR_JOB, t)),
        lambda t: whole(left2, ket_at(FAR_JOB, t)),
        inside,
    )
    back = packed_sum(
        zero,
        lambda t: whole(left2, bra_at(BACK_JOB, t)),
        lambda t: whole_far(ket_at(BACK_JOB, t)),
        inside,
    )

    @pl.when(core == 1)
    def _():
        along_row()

    for cut in range(CUTS):
        swap_far(0, cut).wait_recv()
        swap_far(1, cut).wait_recv()
    far = packed_sum(
        far,
        lambda t: whole(far_in.at[0], t),
        lambda t: whole(left2, far_ket_at(FAR_JOB, t)),
        cross,
    )
    keep(FAR_JOB, far)
    back = packed_sum(
        back,
        lambda t: whole(left2, bra_at(BACK_JOB, inside + t)),
        lambda t: whole(far_in.at[1], t),
        cross,
    )
    keep(BACK_JOB, back)
    for slot in (4, 5, 6, 7):
        result(slot).start()

    @pl.when(quad == 3)
    def _():
        more = zero
        for turn in LEFT:
            hop_extra(turn).wait_recv()
            more = packed_sum(
                more,
                lambda t: whole(packed.at[1 - half], bra_at(NEXT_JOB, turn * cross + t)),
                lambda t: extra[turn, t],
                cross,
            )
        keep(NEXT_JOB, parts[NEXT_JOB].reshape(zero.shape) + more)
        result(1).start()

    @pl.when(quad == 0)
    def _():
        total = zero
        for turn in RIGHT:
            hop_extra(turn).wait_recv()
            total = packed_sum(
                total,
                lambda t: extra[turn, t],
                (lambda t: whole(packed.at[half], ket_at(PREV_JOB, turn * cross + t)))
                if turn * cross < inside else (lambda t: cross_in[1, t]),
                cross,
            )
        keep(PREV_JOB, total)
        result(2).start()
        result(3).start()

    for slot in range(len(RESULTS)):
        result(slot).wait_recv()
    found = [
        parts[ROW_JOB, ga] + inbox[0],
        (parts[NEXT_JOB, ga] + inbox[1]) + (inbox[2] + inbox[3]),
        (inbox[4] + inbox[5]) + (inbox[6] + inbox[7]),
    ]
    for b in range(columns):
        target = jnp.broadcast_to(neighbour[:, b : b + 1], found[0].shape)
        chosen = jnp.where(
            target == at(steps[0]), found[0], jnp.where(target == at(steps[1]), found[1], found[2])
        )
        out[b, 0] = chosen[:, :bands]
        out[b, 1] = chosen[:, bands:]

    def drain(c):
        row_direct(c).wait_send()

        @pl.when((core == 1) & ((place < row - 1) | (c == 0)))
        def _():
            relayed(c).wait_send()

    each(drain)
    for cut in range(CUTS):
        hop_right(cut).wait_send()
        hop_left(cut).wait_send()
        on_right(cut).wait_send()
        on_left(cut).wait_send()
        swap_far(0, cut).wait_send()
        swap_far(1, cut).wait_send()
    for i in range(3):
        send_shift(i).wait_send()

    @pl.when(quad == 3)
    def _():
        for turn in RIGHT:
            hop_extra(turn).wait_send()

    @pl.when(quad == 0)
    def _():
        for turn in LEFT:
            hop_extra(turn).wait_send()

    @pl.when(beside == 3)
    def _():
        for turn in RIGHT_BESIDE:
            extra_back(turn).wait_send()

    @pl.when(beside == 0)
    def _():
        for turn in LEFT_BESIDE:
            extra_back(turn).wait_send()

    @pl.when(between)
    def _():
        from_via().wait_send()


    @pl.when(needs_row)
    def _():
        swap_row().wait_send()

    for i in range(2):
        swap(i).wait_send()
    for slot in range(len(RESULTS)):
        result(slot).wait_send()


def on_device(coeffs, neighbour, shift_id, block_map):
    _, blocks, _, bands, lanes = coeffs.shape
    columns = neighbour.shape[1]
    n_ka = lax.axis_size("ka")
    row = n_ka // 8
    cross = 2 * max(1, blocks // 12)
    def half_buffer(*lead):
        return pltpu.VMEM((*lead, bands, lanes), jnp.bfloat16)

    def cut_buffer(*lead):
        return pltpu.VMEM((*lead, bands // CUTS, lanes), jnp.bfloat16)

    def whole_buffer(*lead):
        return pltpu.VMEM((*lead, 2 * bands, lanes), jnp.bfloat16)

    found = pl.pallas_call(
        functools.partial(kernel, n_ka, row, cross),
        out_shape=jax.ShapeDtypeStruct((columns, 2, bands // 2, bands), jnp.float32),
        in_specs=[
            pl.BlockSpec(memory_space=pltpu.VMEM),
            pl.BlockSpec(memory_space=pltpu.VMEM),
            pl.BlockSpec(memory_space=pltpu.VMEM),
            pl.BlockSpec(memory_space=pl.ANY),
        ],
        out_specs=pl.BlockSpec(memory_space=pltpu.VMEM),
        scratch_shapes=[
            pltpu.VMEM((2, 8, lanes), jnp.int32),
            pltpu.VMEM((3, 8, lanes), jnp.int32),
            pltpu.VMEM((16, lanes), jnp.int32),
            pltpu.SMEM((16, lanes), jnp.int32),
            whole_buffer(blocks),
            cut_buffer(2, CUTS, blocks),
            cut_buffer(CUTS, blocks),
            *[cut_buffer(blocks) for _ in range(CUTS)],
            cut_buffer(CUTS, blocks), cut_buffer(CUTS, blocks),
            half_buffer(TURNS, cross), half_buffer(TURNS, cross), half_buffer(TURNS, cross),
            whole_buffer(blocks), whole_buffer(blocks // CHUNKS), whole_buffer(blocks),
            whole_buffer(cross), whole_buffer(cross),
            half_buffer(2, cross), half_buffer(2, cross),
            cut_buffer(2, CUTS, cross), cut_buffer(2, CUTS, cross),
            pltpu.VMEM((2 * bands, 2 * bands), jnp.float32),
            pltpu.VMEM((5, 2, bands // 2, 2 * bands), jnp.float32),
            pltpu.VMEM((8, bands // 2, 2 * bands), jnp.float32),
            pltpu.SemaphoreType.DMA((5, CHUNKS)),
            pltpu.SemaphoreType.DMA((8, CUTS)),
            pltpu.SemaphoreType.DMA((2, 3)),
            pltpu.SemaphoreType.DMA,
            pltpu.SemaphoreType.DMA((2,)),
            pltpu.SemaphoreType.DMA((4, TURNS)),
            pltpu.SemaphoreType.DMA((2,)),
            pltpu.SemaphoreType.DMA((2, 2)),
            pltpu.SemaphoreType.DMA((2, 2, CUTS)),
            pltpu.SemaphoreType.DMA((2, 8)),
        ],
        compiler_params=pltpu.CompilerParams(
            collective_id=0, has_side_effects=True, vmem_limit_bytes=61 * 2**20
        ),
        name="overlaps",
    )(neighbour, shift_id, block_map, coeffs.reshape(blocks, 2 * bands, lanes))
    return found[None]


def solution(mesh):
    in_specs = (P("ka", "ga", None, None, None), P("ka", None), P("ka", None), P())
    out_specs = P("ka", None, None, "ga", None)
    return jax.shard_map(
        on_device, mesh=mesh, in_specs=in_specs, out_specs=out_specs, check_vma=False
    )
```

```python
import functools

import jax
import jax.numpy as jnp
from jax import lax
from jax.experimental import pallas as pl
from jax.experimental.pallas import tpu as pltpu
from jax.sharding import PartitionSpec as P

MESH = pl.DeviceIdType.MESH
CHUNKS = 8
CUTS = 4
TURNS = 6
OWN_TURNS, ASIDE_TURNS = (0, 1, 2), (3, 4, 5)
PACK = 5
STEP = 20
CONTRACT = (((1,), (1,)), ((), ()))

LOAD, ROW_SENT, RELAY_IN, RELAY_SENT, ROW_IN = range(5)
RIGHT1_SENT, RIGHT1_IN, RIGHT2_SENT, RIGHT2_IN = range(4)
LEFT1_SENT, LEFT1_IN, LEFT2_SENT, LEFT2_IN = range(4, 8)
ROW_JOB, NEXT_JOB, PREV_JOB, FAR_JOB, BACK_JOB = range(5)
JOBS = 5


def flipped(block):
    half = block.shape[1] // 2
    return jnp.concatenate([block[:, half:], -block[:, :half]], axis=1)


def kernel(
    n_ka, row, cross, neighbour, shift_id, block_map, coeffs, out,
    shifts_out, shifts_in, table_rows, table, own, packed, right1, right2_0, right2_1, right2_2, right2_3, left1, left2,
    extra, extra_out, extra_via, relay, via, via_below, ahead,
    row_out, row_in, cross_out, cross_in, far_out, far_in, row_total, parts, inbox,
    chunk_sem, hop_sem, shift_sem, table_sem, via_sem, extra_sem, row_cross_sem, cross_sem,
    far_sem, result_sem,
):
    blocks = own.shape[0]
    bands = own.shape[1] // 2
    lanes = own.shape[2]
    deep = bands // CUTS
    right2 = (right2_0, right2_1, right2_2, right2_3)
    size = blocks // CHUNKS
    inside = blocks - cross
    ka = lax.axis_index("ka")
    ga = lax.axis_index("ga")
    other = 1 - ga
    core = lax.rem(ka, 2)
    place = lax.rem(ka, row)
    odd = lax.rem(place // 4, 2)
    aside = 4 - 8 * odd
    plane = lax.rem(ka // row + 2 * core + odd, 8)
    beside = lax.rem(ka // row + 2 * core + 1 - odd, 4)
    quad = lax.rem(plane, 4)
    half = plane // 4
    needs_row = (core == 0) | (place == row - 1)
    next_half = lax.rem(plane + 1, 8) // 4

    def at(step):
        return lax.rem(ka + n_ka + step, n_ka)

    def part(c):
        return pl.ds(c * size, size)

    def remote(source, target, sent, arrived, device):
        return pltpu.make_async_remote_copy(
            src_ref=source, dst_ref=target, send_sem=sent, recv_sem=arrived,
            device_id=device, device_id_type=MESH,
        )

    def load(i):
        lines = pl.ds((i // 2 + lax.rem(i, 2) * CUTS) * deep, deep)
        return pltpu.make_async_copy(
            coeffs.at[:, lines], own.at[:, lines], chunk_sem.at[LOAD, i]
        )

    def row_direct(c):
        return remote(
            own.at[part(c)], ahead.at[part(c)],
            chunk_sem.at[ROW_SENT, c], chunk_sem.at[ROW_IN, c], (at(-1), ga),
        )

    def row_relayed(c):
        return remote(
            own.at[part(c)], relay.at[part(c)],
            chunk_sem.at[ROW_SENT, c], chunk_sem.at[RELAY_IN, c], (at(-1), other),
        )

    def relayed(c):
        return remote(
            relay.at[part(c)], ahead.at[part(c)],
            chunk_sem.at[RELAY_SENT, c], chunk_sem.at[ROW_IN, c], (ka, other),
        )

    def hop(source, target, sent, cut, step):
        return remote(
            source, target, hop_sem.at[sent, cut], hop_sem.at[sent + 1, cut], (at(step * row), ga)
        )

    def hop_right(cut):
        return hop(packed.at[half, cut], right1.at[cut], RIGHT1_SENT, cut, 1)

    def hop_left(cut):
        return hop(packed.at[1 - half, cut], left1.at[cut], LEFT1_SENT, cut, -1)

    def on_right(cut):
        return hop(right1.at[cut], right2[cut], RIGHT2_SENT, cut, 1)

    def on_left(cut):
        return hop(left1.at[cut], left2.at[cut], LEFT2_SENT, cut, -1)

    def hop_extra(turn):
        return remote(
            extra_out.at[turn], extra.at[turn],
            extra_sem.at[0, turn], extra_sem.at[1, turn], (at(row), ga),
        )

    def extra_aside(turn):
        return remote(
            extra_out.at[turn], extra_via.at[turn],
            extra_sem.at[0, turn], extra_sem.at[2, turn], (at(aside), ga),
        )

    def extra_back(turn):
        return remote(
            extra_via.at[turn], extra.at[turn],
            extra_sem.at[3, turn], extra_sem.at[1, turn], (at(aside + row), ga),
        )

    def via_side(c):
        return jnp.where(lax.rem(c, 2) == 1, other, ga)

    def to_via(c):
        return remote(
            own.at[part(c)], via, chunk_sem.at[ROW_SENT, c], via_sem.at[0],
            (at(2 * c), via_side(c)),
        )

    def down_via():
        return remote(via, via_below, via_sem.at[1], via_sem.at[2], (at(-row), ga))

    def from_via():
        c = place // 2
        return remote(
            via_below, ahead.at[part(c)], via_sem.at[3], chunk_sem.at[ROW_IN, c],
            (at(row - 1 - place), via_side(c)),
        )

    def swap_row():
        return remote(row_out, row_in, row_cross_sem.at[0], row_cross_sem.at[1], (ka, other))

    def swap(i):
        return remote(
            cross_out.at[i], cross_in.at[i], cross_sem.at[0, i], cross_sem.at[1, i], (ka, other)
        )

    def swap_far(i, cut):
        return remote(
            far_out.at[i, cut], far_in.at[i, cut],
            far_sem.at[0, i, cut], far_sem.at[1, i, cut], (ka, other),
        )

    def result(slot):
        job, step, same = RESULTS[slot]
        side = ga if same else other
        return remote(
            parts.at[job, side], inbox.at[slot],
            result_sem.at[0, slot], result_sem.at[1, slot], (at(step * row), side),
        )

    RESULTS = (
        (ROW_JOB, 0, False), (NEXT_JOB, 0, False),
        (PREV_JOB, -1, True), (PREV_JOB, -1, False),
        (FAR_JOB, -2, True), (FAR_JOB, -2, False),
        (BACK_JOB, 2, True), (BACK_JOB, 2, False),
    )

    def each(body):
        def run(c, carry):
            body(c)
            return carry
        lax.fori_loop(0, CHUNKS, run, 0)

    def bra_at(job, t):
        return table[job, t]

    def ket_at(job, t):
        return table[JOBS + job, t]

    def far_ket_at(job, t):
        return table[2 * JOBS + job, inside + t]

    def whole(source, index):
        return jnp.concatenate([source[cut, index] for cut in range(CUTS)], axis=0)

    def whole_far(index):
        return jnp.concatenate([right2[cut][index] for cut in range(CUTS)], axis=0)

    def gather(target, pick):
        def run(t, carry):
            for u in range(PACK):
                target[t * PACK + u] = pick(t * PACK + u)
            return carry
        lax.fori_loop(0, cross // PACK, run, 0)

    def whole_sum(total, bra, ket, count):
        def run(s, total):
            left = jnp.concatenate([bra(s * STEP + u) for u in range(STEP)], axis=1)
            right = jnp.concatenate([ket(s * STEP + u) for u in range(STEP)], axis=1)
            return total + lax.dot_general(
                left, right, CONTRACT, preferred_element_type=jnp.float32
            )
        return lax.fori_loop(0, count // STEP, run, total)

    def packed_sum(total, bra, ket, count):
        def run(s, total):
            left = jnp.concatenate([bra(s * STEP + u) for u in range(STEP)], axis=1)
            kets = [ket(s * STEP + u) for u in range(STEP)]
            right = jnp.concatenate(
                [jnp.concatenate(kets, axis=1),
                 jnp.concatenate([flipped(k) for k in kets], axis=1)], axis=0
            )
            return total + lax.dot_general(
                left, right, CONTRACT, preferred_element_type=jnp.float32
            )
        return lax.fori_loop(0, count // STEP, run, total)

    def keep(job, total):
        parts[job] = total.reshape(parts.shape[1:])

    zero = jnp.zeros((bands, 2 * bands), jnp.float32)

    each(lambda c: load(c).start())

    tile = (8, lanes)
    columns = neighbour.shape[1]
    targets = [jnp.broadcast_to(neighbour[:, b : b + 1], tile) for b in range(columns)]
    steps = (1, row, n_ka // 2)

    def shift_of(step):
        found = jnp.zeros(tile, jnp.int32)
        for b in range(columns):
            moved = jnp.broadcast_to(shift_id[:, b : b + 1], tile)
            found = found + jnp.where(targets[b] == at(step), moved, 0)
        return found

    row_shift, next_shift, far_shift = [shift_of(step) for step in steps]
    shifts_out[0] = next_shift
    shifts_out[1] = far_shift

    def send_shift(i):
        return remote(
            shifts_out.at[min(i, 1)], shifts_in.at[i],
            shift_sem.at[0, i], shift_sem.at[1, i], (at((row, 2 * row, -2 * row)[i]), ga),
        )

    barrier = pltpu.get_barrier_semaphore()
    meet = [
        (ka, other), (at(row), ga), (at(-row), ga), (at(row), other), (at(-row), other),
        (at(2 * row), ga), (at(-2 * row), ga), (at(2 * row), other), (at(-2 * row), other),
        (at(-1), jnp.where(core == 1, ga, other)), (at(1), jnp.where(core == 0, ga, other)),
        (at(aside), ga), (at(aside + row), ga), (at(aside - row), ga),
    ]
    paths = row // 2

    def greet(device):
        pl.semaphore_signal(barrier, inc=1, device_id=device, device_id_type=MESH)

    for device in meet:
        greet(device)

    @pl.when(place == 0)
    def _():
        for p in range(1, paths):
            greet((at(2 * p), via_side(p)))

    @pl.when(place == row - 1)
    def _():
        for p in range(1, paths):
            greet((at(1 - row + 2 * p), via_side(p)))

    between = (core == 0) & (place > 0)

    @pl.when(between)
    def _():
        greet((at(-place), via_side(place // 2)))
        greet((at(row - 1 - place), via_side(place // 2)))

    def load_cut(cut):
        load(2 * cut).wait()
        load(2 * cut + 1).wait()

    def pack_cut(cut):
        def pack(t, carry):
            for u in range(STEP):
                j = t * STEP + u
                real = own[j, pl.ds(cut * deep, deep), :]
                imag = own[j, pl.ds(bands + cut * deep, deep), :]
                mid = lanes // 2
                packed[0, cut, j] = jnp.concatenate([real[:, :mid], imag[:, :mid]], axis=1)
                packed[1, cut, j] = jnp.concatenate([real[:, mid:], imag[:, mid:]], axis=1)
            return carry
        lax.fori_loop(0, blocks // STEP, pack, 0)

    load_cut(0)
    pack_cut(0)
    ends = (place == 0) | (place == row - 1)
    pl.semaphore_wait(
        barrier, len(meet) + jnp.where(ends, paths - 1, 0) + jnp.where(between, 2, 0)
    )
    for i in range(3):
        send_shift(i).start()

    def make_table():
        lane = lax.broadcasted_iota(jnp.int32, (lanes, lanes), 1)
        line = lax.broadcasted_iota(jnp.int32, (lanes, lanes), 0)
        maps = [
            jnp.concatenate(
                [block_map[:, a * blocks : (a + 1) * blocks],
                 jnp.zeros((block_map.shape[0], lanes - blocks), jnp.int32)], axis=1
            )
            for a in range(2)
        ]
        maps = [jnp.where(ga == a, maps[0], maps[1]) for a in range(2)]
        shifts = [row_shift, next_shift] + [shifts_in[i] for i in range(3)]
        choice = lax.broadcasted_iota(jnp.int32, tile, 0)
        rows = [
            jnp.sum(jnp.where(shift == choice, each_map, 0), axis=0, keepdims=True)
            for each_map in maps for shift in shifts
        ]
        rows = jnp.concatenate(rows + [jnp.zeros((16 - 2 * JOBS, lanes), jnp.int32)], axis=0)
        number = lax.broadcasted_iota(jnp.int32, rows.shape, 0)
        spot = lax.broadcasted_iota(jnp.int32, rows.shape, 1)
        source = jnp.where(rows >= blocks, 1, 0)
        same = jnp.where(source == jnp.where(number < JOBS, ga, other), 1, 0)
        local = rows - blocks * source
        same_t = same.T
        kept = [
            jnp.sum(jnp.where(line < lane, same_t[:, r : r + 1], 0), axis=0, keepdims=True)
            for r in range(2 * JOBS)
        ]
        kept = jnp.concatenate(kept + [jnp.zeros((16 - 2 * JOBS, lanes), jnp.int32)], axis=0)
        rank = jnp.where(same == 1, kept, inside + spot - kept)
        rank_t = jnp.where(spot < blocks, rank, -1).T
        local_t = local.T
        hits = [rank_t[:, r : r + 1] == lane for r in range(2 * JOBS)]
        lists = [jnp.sum(jnp.where(hits[r], line, 0), axis=0, keepdims=True) for r in range(JOBS)]
        lists += [
            jnp.sum(jnp.where(hits[r], local_t[:, r : r + 1], 0), axis=0, keepdims=True)
            for r in range(2 * JOBS)
        ]
        lists += [jnp.zeros((1, lanes), jnp.int32)]
        table_rows[...] = jnp.concatenate(lists, axis=0)

    def first_sends(c):
        @pl.when(core == 1)
        def _():
            row_direct(c).start()

        @pl.when((core == 0) & ((place > 0) | (c == 0)))
        def _():
            row_relayed(c).start()

        @pl.when((place == 0) & (c > 0))
        def _():
            to_via(c).start()

    hop_right(0).start()
    hop_left(0).start()
    for cut in range(1, CUTS):
        load_cut(cut)
    each(first_sends)
    pack_cut(1)
    for cut in range(1, CUTS):
        if cut + 1 < CUTS:
            pack_cut(cut + 1)
        hop_right(cut).start()
        hop_left(cut).start()
    for i in range(3):
        send_shift(i).wait_recv()
    make_table()
    fetch = pltpu.make_async_copy(table_rows, table, table_sem)
    fetch.start()
    fetch.wait()
    gather(cross_out.at[0], lambda t: whole(packed.at[1 - next_half], bra_at(NEXT_JOB, inside + t)))
    gather(cross_out.at[1], lambda t: whole(packed.at[half], far_ket_at(PREV_JOB, t)))

    @pl.when(needs_row)
    def _():
        gather(row_out, lambda t: own[bra_at(ROW_JOB, inside + t)])
        swap_row().start()

    swap(0).start()
    swap(1).start()

    @pl.when(quad == 3)
    def _():
        for turn in ASIDE_TURNS + OWN_TURNS:
            gather(
                extra_out.at[turn],
                lambda t: whole(packed.at[1 - half], bra_at(NEXT_JOB, turn * cross + t)),
            )
        for turn in ASIDE_TURNS:
            extra_aside(turn).start()

    def relay_on(c):
        row_relayed(c).wait_recv()
        relayed(c).start()

    for cut in range(CUTS):
        hop_right(cut).wait_recv()
        on_right(cut).start()
        hop_left(cut).wait_recv()

        if cut == 1:
            @pl.when(between)
            def _():
                to_via(0).wait_recv()
                down_via().start()

        on_left(cut).start()

        @pl.when((core == 1) & (place < row - 1))
        def _(cut=cut):
            for c in range(cut * CHUNKS // CUTS, (cut + 1) * CHUNKS // CUTS):
                relay_on(c)

        if cut == 1:
            @pl.when(place == row - 1)
            def _():
                relay_on(0)

    @pl.when(quad == 3)
    def _():
        for turn in OWN_TURNS:
            hop_extra(turn).start()

    @pl.when(beside == 3)
    def _():
        for turn in ASIDE_TURNS:
            extra_aside(turn).wait_recv()
            extra_back(turn).start()

    swap(0).wait_recv()
    total = packed_sum(
        zero,
        lambda t: whole(packed.at[1 - next_half], bra_at(NEXT_JOB, t)),
        lambda t: whole(left1, ket_at(NEXT_JOB, t)),
        inside,
    )
    total = packed_sum(
        total, lambda t: cross_in[0, t], lambda t: whole(left1, far_ket_at(NEXT_JOB, t)), cross
    )
    keep(NEXT_JOB, total)

    swap(1).wait_recv()

    @pl.when(quad != 0)
    def _():
        total = packed_sum(
            zero,
            lambda t: whole(right1, bra_at(PREV_JOB, t)),
            lambda t: whole(packed.at[half], ket_at(PREV_JOB, t)),
            inside,
        )
        total = packed_sum(
            total,
            lambda t: whole(right1, bra_at(PREV_JOB, inside + t)),
            lambda t: cross_in[1, t],
            cross,
        )
        keep(PREV_JOB, total)

    result(1).start()

    def along_row():
        each(lambda c: row_direct(c).wait_recv())
        row_total[...] = whole_sum(
            jnp.zeros(row_total.shape, jnp.float32),
            lambda t: own[bra_at(ROW_JOB, t)],
            lambda t: ahead[ket_at(ROW_JOB, t)],
            inside,
        )

        @pl.when(needs_row)
        def _():
            swap_row().wait_recv()
            row_total[...] = whole_sum(
                row_total[...], lambda t: row_in[t], lambda t: ahead[far_ket_at(ROW_JOB, t)], cross
            )

        @pl.when(jnp.logical_not(needs_row))
        def _():
            row_total[...] = whole_sum(
                row_total[...],
                lambda t: own[bra_at(ROW_JOB, inside + t)],
                lambda t: relay[ket_at(ROW_JOB, inside + t)],
                cross,
            )

        lower = row_total[pl.ds(bands, bands)]
        keep(
            ROW_JOB,
            row_total[pl.ds(0, bands)]
            + jnp.concatenate([lower[:, bands:], -lower[:, :bands]], axis=1),
        )
        result(0).start()

    @pl.when(core == 0)
    def _():
        along_row()

    def far_swaps(cut):
        on_right(cut).wait_recv()
        gather(far_out.at[0, cut], lambda t: right2[cut][bra_at(FAR_JOB, inside + t)])
        gather(far_out.at[1, cut], lambda t: right2[cut][far_ket_at(BACK_JOB, t)])
        swap_far(0, cut).start()
        swap_far(1, cut).start()

    far_swaps(0)

    @pl.when(between)
    def _():
        down_via().wait_recv()
        from_via().start()

    @pl.when(quad != 0)
    def _():
        result(2).start()
        result(3).start()

    for cut in range(1, CUTS):
        if cut == CUTS - 1:
            @pl.when((core == 1) & (place > 1))
            def _():
                along_row()

        far_swaps(cut)

    def previous_extra():
        total = zero
        for turn in range(TURNS):
            hop_extra(turn).wait_recv()
            total = packed_sum(
                total,
                lambda t: extra[turn, t],
                (lambda t: whole(packed.at[half], ket_at(PREV_JOB, turn * cross + t)))
                if turn * cross < inside else (lambda t: cross_in[1, t]),
                cross,
            )
        keep(PREV_JOB, total)
        result(2).start()
        result(3).start()

    for cut in range(CUTS):
        on_left(cut).wait_recv()
    far = packed_sum(
        zero,
        lambda t: whole_far(bra_at(FAR_JOB, t)),
        lambda t: whole(left2, ket_at(FAR_JOB, t)),
        inside,
    )
    back = packed_sum(
        zero,
        lambda t: whole(left2, bra_at(BACK_JOB, t)),
        lambda t: whole_far(ket_at(BACK_JOB, t)),
        inside,
    )


    @pl.when(place == 1)
    def _():
        along_row()

    for cut in range(CUTS):
        swap_far(0, cut).wait_recv()
        swap_far(1, cut).wait_recv()
    far = packed_sum(
        far,
        lambda t: whole(far_in.at[0], t),
        lambda t: whole(left2, far_ket_at(FAR_JOB, t)),
        cross,
    )
    keep(FAR_JOB, far)
    back = packed_sum(
        back,
        lambda t: whole(left2, bra_at(BACK_JOB, inside + t)),
        lambda t: whole(far_in.at[1], t),
        cross,
    )
    keep(BACK_JOB, back)
    for slot in (4, 5, 6, 7):
        result(slot).start()

    @pl.when(quad == 0)
    def _():
        previous_extra()

    for slot in range(len(RESULTS)):
        result(slot).wait_recv()
    found = [
        parts[ROW_JOB, ga] + inbox[0],
        (parts[NEXT_JOB, ga] + inbox[1]) + (inbox[2] + inbox[3]),
        (inbox[4] + inbox[5]) + (inbox[6] + inbox[7]),
    ]
    for b in range(columns):
        target = jnp.broadcast_to(neighbour[:, b : b + 1], found[0].shape)
        chosen = jnp.where(
            target == at(steps[0]), found[0], jnp.where(target == at(steps[1]), found[1], found[2])
        )
        out[b, 0] = chosen[:, :bands]
        out[b, 1] = chosen[:, bands:]

    def drain(c):
        row_direct(c).wait_send()

        @pl.when((core == 1) & ((place < row - 1) | (c == 0)))
        def _():
            relayed(c).wait_send()

    each(drain)
    for cut in range(CUTS):
        hop_right(cut).wait_send()
        hop_left(cut).wait_send()
        on_right(cut).wait_send()
        on_left(cut).wait_send()
        swap_far(0, cut).wait_send()
        swap_far(1, cut).wait_send()
    for i in range(3):
        send_shift(i).wait_send()

    @pl.when(quad == 3)
    def _():
        for turn in range(TURNS):
            hop_extra(turn).wait_send()

    @pl.when(beside == 3)
    def _():
        for turn in ASIDE_TURNS:
            extra_back(turn).wait_send()

    @pl.when(between)
    def _():
        down_via().wait_send()
        from_via().wait_send()


    @pl.when(needs_row)
    def _():
        swap_row().wait_send()

    for i in range(2):
        swap(i).wait_send()
    for slot in range(len(RESULTS)):
        result(slot).wait_send()


def on_device(coeffs, neighbour, shift_id, block_map):
    _, blocks, _, bands, lanes = coeffs.shape
    columns = neighbour.shape[1]
    n_ka = lax.axis_size("ka")
    row = n_ka // 8
    cross = 2 * max(1, blocks // 12)
    def half_buffer(*lead):
        return pltpu.VMEM((*lead, bands, lanes), jnp.bfloat16)

    def cut_buffer(*lead):
        return pltpu.VMEM((*lead, bands // CUTS, lanes), jnp.bfloat16)

    def whole_buffer(*lead):
        return pltpu.VMEM((*lead, 2 * bands, lanes), jnp.bfloat16)

    found = pl.pallas_call(
        functools.partial(kernel, n_ka, row, cross),
        out_shape=jax.ShapeDtypeStruct((columns, 2, bands // 2, bands), jnp.float32),
        in_specs=[
            pl.BlockSpec(memory_space=pltpu.VMEM),
            pl.BlockSpec(memory_space=pltpu.VMEM),
            pl.BlockSpec(memory_space=pltpu.VMEM),
            pl.BlockSpec(memory_space=pl.ANY),
        ],
        out_specs=pl.BlockSpec(memory_space=pltpu.VMEM),
        scratch_shapes=[
            pltpu.VMEM((2, 8, lanes), jnp.int32),
            pltpu.VMEM((3, 8, lanes), jnp.int32),
            pltpu.VMEM((16, lanes), jnp.int32),
            pltpu.SMEM((16, lanes), jnp.int32),
            whole_buffer(blocks),
            cut_buffer(2, CUTS, blocks),
            cut_buffer(CUTS, blocks),
            *[cut_buffer(blocks) for _ in range(CUTS)],
            cut_buffer(CUTS, blocks), cut_buffer(CUTS, blocks),
            half_buffer(TURNS, cross), half_buffer(TURNS, cross), half_buffer(TURNS, cross),
            whole_buffer(blocks), whole_buffer(blocks // CHUNKS), whole_buffer(blocks // CHUNKS), whole_buffer(blocks),
            whole_buffer(cross), whole_buffer(cross),
            half_buffer(2, cross), half_buffer(2, cross),
            cut_buffer(2, CUTS, cross), cut_buffer(2, CUTS, cross),
            pltpu.VMEM((2 * bands, 2 * bands), jnp.float32),
            pltpu.VMEM((5, 2, bands // 2, 2 * bands), jnp.float32),
            pltpu.VMEM((8, bands // 2, 2 * bands), jnp.float32),
            pltpu.SemaphoreType.DMA((5, CHUNKS)),
            pltpu.SemaphoreType.DMA((8, CUTS)),
            pltpu.SemaphoreType.DMA((2, 3)),
            pltpu.SemaphoreType.DMA,
            pltpu.SemaphoreType.DMA((4,)),
            pltpu.SemaphoreType.DMA((4, TURNS)),
            pltpu.SemaphoreType.DMA((2,)),
            pltpu.SemaphoreType.DMA((2, 2)),
            pltpu.SemaphoreType.DMA((2, 2, CUTS)),
            pltpu.SemaphoreType.DMA((2, 8)),
        ],
        compiler_params=pltpu.CompilerParams(
            collective_id=0, has_side_effects=True, vmem_limit_bytes=61 * 2**20
        ),
        name="overlaps",
    )(neighbour, shift_id, block_map, coeffs.reshape(blocks, 2 * bands, lanes))
    return found[None]


def solution(mesh):
    in_specs = (P("ka", "ga", None, None, None), P("ka", None), P("ka", None), P())
    out_specs = P("ka", None, None, "ga", None)
    return jax.shard_map(
        on_device, mesh=mesh, in_specs=in_specs, out_specs=out_specs, check_vma=False
    )
```

```python
import functools

import jax
import jax.numpy as jnp
from jax import lax
from jax.experimental import pallas as pl
from jax.experimental.pallas import tpu as pltpu
from jax.sharding import PartitionSpec as P

MESH = pl.DeviceIdType.MESH
CHUNKS = 8
CUTS = 4
TURNS = 6
LEFT_OWN, LEFT_ASIDE = (0,), (1,)
RIGHT_OWN, RIGHT_ASIDE = (2, 3), (4, 5)
LEFT = LEFT_OWN + LEFT_ASIDE
RIGHT = RIGHT_OWN + RIGHT_ASIDE
PACK = 5
STEP = 20
CONTRACT = (((1,), (1,)), ((), ()))

LOAD, ROW_SENT, RELAY_IN, RELAY_SENT, ROW_IN = range(5)
RIGHT1_SENT, RIGHT1_IN, RIGHT2_SENT, RIGHT2_IN = range(4)
LEFT1_SENT, LEFT1_IN, LEFT2_SENT, LEFT2_IN = range(4, 8)
ROW_JOB, NEXT_JOB, PREV_JOB, FAR_JOB, BACK_JOB, WRAP_JOB = range(6)
JOBS = 6


def flipped(block):
    half = block.shape[1] // 2
    return jnp.concatenate([block[:, half:], -block[:, :half]], axis=1)


def kernel(
    n_ka, row, cross, neighbour_in, shift_in, map_in, coeffs, out,
    neighbour, shift_id, block_map,    shifts_out, shifts_in, table_rows, table, own, packed, right1, right2_0, right2_1, right2_2, right2_3, left1, left2,
    extra, extra_out, extra_via, relay, ahead, near, pass_a, pass_b, wrap_out, wrap_in,
    row_out, row_in, cross_out, cross_in, far_out, far_in, row_total, parts, inbox,
    small_sem, chunk_sem, hop_sem, shift_sem, table_sem, near_sem, wrap_sem, extra_sem, row_cross_sem, cross_sem,
    far_sem, result_sem,
):
    blocks = own.shape[0]
    bands = own.shape[1] // 2
    lanes = own.shape[2]
    deep = bands // CUTS
    right2 = (right2_0, right2_1, right2_2, right2_3)
    size = blocks // CHUNKS
    inside = blocks - cross
    ka = lax.axis_index("ka")
    ga = lax.axis_index("ga")
    other = 1 - ga
    core = lax.rem(ka, 2)
    place = lax.rem(ka, row)
    odd = lax.rem(place // 4, 2)
    aside = 4 - 8 * odd
    turned = jnp.where(odd == 1, 3 - 2 * core, 2 * core)
    plane = lax.rem(ka // row + turned, 8)
    beside = lax.rem(ka // row + 3 - turned, 4)
    first = place == 0
    last = place == row - 1
    quad = lax.rem(plane, 4)
    half = plane // 4
    needs_row = (core == 0) | last
    next_half = lax.rem(plane + 1, 8) // 4

    def at(step):
        return lax.rem(ka + n_ka + step, n_ka)

    def part(c):
        return pl.ds(c * size, size)

    def remote(source, target, sent, arrived, device):
        return pltpu.make_async_remote_copy(
            src_ref=source, dst_ref=target, send_sem=sent, recv_sem=arrived,
            device_id=device, device_id_type=MESH,
        )

    def load(i):
        lines = pl.ds((i // 2 + lax.rem(i, 2) * CUTS) * deep, deep)
        return pltpu.make_async_copy(
            coeffs.at[:, lines], own.at[:, lines], chunk_sem.at[LOAD, i]
        )

    def row_direct(c):
        return remote(
            own.at[part(c)], ahead.at[part(c)],
            chunk_sem.at[ROW_SENT, c], chunk_sem.at[ROW_IN, c], (at(-1), ga),
        )

    def row_relayed(c):
        return remote(
            own.at[part(c)], relay.at[part(c)],
            chunk_sem.at[ROW_SENT, c], chunk_sem.at[RELAY_IN, c], (at(-1), other),
        )

    def relayed(c):
        return remote(
            relay.at[part(c)], ahead.at[part(c)],
            chunk_sem.at[RELAY_SENT, c], chunk_sem.at[ROW_IN, c], (ka, other),
        )

    def hop(source, target, sent, cut, step):
        return remote(
            source, target, hop_sem.at[sent, cut], hop_sem.at[sent + 1, cut], (at(step * row), ga)
        )

    def hop_right(cut):
        return hop(packed.at[half, cut], right1.at[cut], RIGHT1_SENT, cut, 1)

    def hop_left(cut):
        return hop(packed.at[1 - half, cut], left1.at[cut], LEFT1_SENT, cut, -1)

    def on_right(cut):
        return hop(right1.at[cut], right2[cut], RIGHT2_SENT, cut, 1)

    def on_left(cut):
        return hop(left1.at[cut], left2.at[cut], LEFT2_SENT, cut, -1)

    def hop_extra(turn):
        return remote(
            extra_out.at[turn], extra.at[turn],
            extra_sem.at[0, turn], extra_sem.at[1, turn],
            (at(-row if turn in LEFT else row), ga),
        )

    def extra_aside(turn):
        return remote(
            extra_out.at[turn], extra_via.at[turn],
            extra_sem.at[0, turn], extra_sem.at[2, turn], (at(aside), ga),
        )

    def extra_back(turn):
        return remote(
            extra_via.at[turn], extra.at[turn],
            extra_sem.at[3, turn], extra_sem.at[1, turn],
            (at(aside + (-row if turn in LEFT else row)), ga),
        )

    def carry_left(cut):
        return remote(
            left1.at[cut], pass_a.at[cut],
            near_sem.at[0, cut], near_sem.at[1, cut], (at(row - 1), other),
        )

    def carry_right(cut):
        return remote(
            right1.at[cut], pass_b.at[cut],
            near_sem.at[2, cut], near_sem.at[3, cut], (ka, other),
        )

    def to_last(cut):
        return remote(
            pass_a.at[cut], near.at[cut], near_sem.at[4, cut], near_sem.at[5, cut], (ka, other)
        )

    def to_first(cut):
        return remote(
            pass_b.at[cut], near.at[cut],
            near_sem.at[6, cut], near_sem.at[5, cut], (at(1 - row), other),
        )

    def swap_wrap():
        return remote(wrap_out, wrap_in, wrap_sem.at[0], wrap_sem.at[1], (ka, other))

    def swap_row():
        return remote(row_out, row_in, row_cross_sem.at[0], row_cross_sem.at[1], (ka, other))

    def swap(i):
        return remote(
            cross_out.at[i], cross_in.at[i], cross_sem.at[0, i], cross_sem.at[1, i], (ka, other)
        )

    def swap_far(i, cut):
        return remote(
            far_out.at[i, cut], far_in.at[i, cut],
            far_sem.at[0, i, cut], far_sem.at[1, i, cut], (ka, other),
        )

    def result(slot):
        job, step, same = RESULTS[slot]
        side = ga if same else other
        return remote(
            parts.at[job, side], inbox.at[slot],
            result_sem.at[0, slot], result_sem.at[1, slot], (at(step), side),
        )

    RESULTS = (
        (ROW_JOB, 0, False), (NEXT_JOB, 0, False),
        (PREV_JOB, -row, True), (PREV_JOB, -row, False),
        (FAR_JOB, -2 * row, True), (FAR_JOB, -2 * row, False),
        (BACK_JOB, 2 * row, True), (BACK_JOB, 2 * row, False),
        (WRAP_JOB, -1, True), (WRAP_JOB, -1, False),
    )
    WRAPPED = (8, 9)

    def each(body):
        def run(c, carry):
            body(c)
            return carry
        lax.fori_loop(0, CHUNKS, run, 0)

    def bra_at(job, t):
        return table[job, t]

    def ket_at(job, t):
        return table[JOBS + job, t]

    def far_ket_at(job, t):
        return table[2 * JOBS + job, inside + t]

    def whole(source, index):
        return jnp.concatenate([source[cut, index] for cut in range(CUTS)], axis=0)

    def whole_far(index):
        return jnp.concatenate([right2[cut][index] for cut in range(CUTS)], axis=0)

    def gather(target, pick):
        def run(t, carry):
            for u in range(PACK):
                target[t * PACK + u] = pick(t * PACK + u)
            return carry
        lax.fori_loop(0, cross // PACK, run, 0)

    def whole_sum(total, bra, ket, count):
        def run(s, total):
            left = jnp.concatenate([bra(s * STEP + u) for u in range(STEP)], axis=1)
            right = jnp.concatenate([ket(s * STEP + u) for u in range(STEP)], axis=1)
            return total + lax.dot_general(
                left, right, CONTRACT, preferred_element_type=jnp.float32
            )
        return lax.fori_loop(0, count // STEP, run, total)

    def packed_step(total, pairs):
        left = jnp.concatenate([bra for bra, _ in pairs], axis=1)
        right = jnp.concatenate(
            [jnp.concatenate([ket for _, ket in pairs], axis=1),
             jnp.concatenate([flipped(ket) for _, ket in pairs], axis=1)], axis=0
        )
        return total + lax.dot_general(
            left, right, CONTRACT, preferred_element_type=jnp.float32
        )

    def packed_sums(totals, sources, count):
        def run(s, totals):
            return tuple(
                packed_step(
                    total, [(bra(s * STEP + u), ket(s * STEP + u)) for u in range(STEP)]
                )
                for total, (bra, ket) in zip(totals, sources)
            )
        return lax.fori_loop(0, count // STEP, run, tuple(totals))

    def packed_sum(total, bra, ket, count):
        return packed_sums((total,), ((bra, ket),), count)[0]

    def keep(job, total):
        parts[job] = total.reshape(parts.shape[1:])

    zero = jnp.zeros((bands, 2 * bands), jnp.float32)

    small = [
        pltpu.make_async_copy(given, held, small_sem.at[i])
        for i, (given, held) in enumerate(
            ((neighbour_in, neighbour), (shift_in, shift_id), (map_in, block_map))
        )
    ]
    for copy in small:
        copy.start()
    each(lambda c: load(c).start())
    for copy in small:
        copy.wait()

    tile = (8, lanes)
    columns = neighbour.shape[1]
    targets = [jnp.broadcast_to(neighbour[:, b : b + 1], tile) for b in range(columns)]
    steps = (1, row, n_ka // 2)

    def shift_of(step):
        found = jnp.zeros(tile, jnp.int32)
        for b in range(columns):
            moved = jnp.broadcast_to(shift_id[:, b : b + 1], tile)
            found = found + jnp.where(targets[b] == at(step), moved, 0)
        return found

    row_shift, next_shift, far_shift = [shift_of(step) for step in steps]
    shifts_out[0] = next_shift
    shifts_out[1] = far_shift
    shifts_out[2] = row_shift

    def send_shift(i):
        return remote(
            shifts_out.at[(0, 1, 1, 2)[i]], shifts_in.at[i],
            shift_sem.at[0, i], shift_sem.at[1, i], (at((row, 2 * row, -2 * row, 1)[i]), ga),
        )

    barrier = pltpu.get_barrier_semaphore()
    meet = [
        (ka, other), (at(row), ga), (at(-row), ga), (at(row), other), (at(-row), other),
        (at(2 * row), ga), (at(-2 * row), ga), (at(2 * row), other), (at(-2 * row), other),
        (at(-1), ga), (at(1), ga), (at(-1), other), (at(1), other),
        (at(aside), ga), (at(aside + row), ga), (at(aside - row), ga),
    ]
    def greet(device):
        pl.semaphore_signal(barrier, inc=1, device_id=device, device_id_type=MESH)

    for device in meet:
        greet(device)

    @pl.when(first)
    def _():
        greet((at(row - 1), other))

    @pl.when(last)
    def _():
        greet((at(1 - row), other))

    def load_cut(cut):
        load(2 * cut).wait()
        load(2 * cut + 1).wait()

    def pack_cut(cut):
        def pack(t, carry):
            for u in range(STEP):
                j = t * STEP + u
                real = own[j, pl.ds(cut * deep, deep), :]
                imag = own[j, pl.ds(bands + cut * deep, deep), :]
                mid = lanes // 2
                packed[0, cut, j] = jnp.concatenate([real[:, :mid], imag[:, :mid]], axis=1)
                packed[1, cut, j] = jnp.concatenate([real[:, mid:], imag[:, mid:]], axis=1)
            return carry
        lax.fori_loop(0, blocks // STEP, pack, 0)

    load_cut(0)
    pack_cut(0)
    pl.semaphore_wait(barrier, len(meet) + jnp.where(first | last, 1, 0))
    for i in range(4):
        send_shift(i).start()

    def make_table():
        lane = lax.broadcasted_iota(jnp.int32, (lanes, lanes), 1)
        line = lax.broadcasted_iota(jnp.int32, (lanes, lanes), 0)
        maps = [
            jnp.concatenate(
                [block_map[:, a * blocks : (a + 1) * blocks],
                 jnp.zeros((block_map.shape[0], lanes - blocks), jnp.int32)], axis=1
            )
            for a in range(2)
        ]
        maps = [jnp.where(ga == a, maps[0], maps[1]) for a in range(2)]
        shifts = [row_shift, next_shift] + [shifts_in[i] for i in range(4)]
        choice = lax.broadcasted_iota(jnp.int32, tile, 0)
        rows = [
            jnp.sum(jnp.where(shift == choice, each_map, 0), axis=0, keepdims=True)
            for each_map in maps for shift in shifts
        ]
        rows = jnp.concatenate(rows + [jnp.zeros((16 - 2 * JOBS, lanes), jnp.int32)], axis=0)
        number = lax.broadcasted_iota(jnp.int32, rows.shape, 0)
        spot = lax.broadcasted_iota(jnp.int32, rows.shape, 1)
        source = jnp.where(rows >= blocks, 1, 0)
        same = jnp.where(source == jnp.where(number < JOBS, ga, other), 1, 0)
        local = rows - blocks * source
        same_t = same.T
        kept = [
            jnp.sum(jnp.where(line < lane, same_t[:, r : r + 1], 0), axis=0, keepdims=True)
            for r in range(2 * JOBS)
        ]
        kept = jnp.concatenate(kept + [jnp.zeros((16 - 2 * JOBS, lanes), jnp.int32)], axis=0)
        rank = jnp.where(same == 1, kept, inside + spot - kept)
        rank_t = jnp.where(spot < blocks, rank, -1).T
        local_t = local.T
        hits = [rank_t[:, r : r + 1] == lane for r in range(2 * JOBS)]
        lists = [jnp.sum(jnp.where(hits[r], line, 0), axis=0, keepdims=True) for r in range(JOBS)]
        lists += [
            jnp.sum(jnp.where(hits[r], local_t[:, r : r + 1], 0), axis=0, keepdims=True)
            for r in range(2 * JOBS)
        ]
        lists += [jnp.zeros((24 - 3 * JOBS, lanes), jnp.int32)]
        table_rows[...] = jnp.concatenate(lists, axis=0)

    def first_sends(c):
        @pl.when(core == 1)
        def _():
            row_direct(c).start()

        @pl.when((core == 0) & (place > 0))
        def _():
            row_relayed(c).start()

    hop_right(0).start()
    hop_left(0).start()
    for cut in range(1, CUTS):
        load_cut(cut)
    each(first_sends)
    pack_cut(1)
    for cut in range(1, CUTS):
        if cut + 1 < CUTS:
            pack_cut(cut + 1)
        hop_right(cut).start()
        hop_left(cut).start()
    for i in range(4):
        send_shift(i).wait_recv()
    make_table()
    fetch = pltpu.make_async_copy(table_rows, table, table_sem)
    fetch.start()
    fetch.wait()
    gather(cross_out.at[0], lambda t: whole(packed.at[1 - next_half], bra_at(NEXT_JOB, inside + t)))
    gather(cross_out.at[1], lambda t: whole(packed.at[half], far_ket_at(PREV_JOB, t)))

    @pl.when(core == 0)
    def _():
        gather(row_out, lambda t: own[bra_at(ROW_JOB, inside + t)])

    @pl.when(last)
    def _():
        gather(
            row_out,
            lambda t: jnp.concatenate(
                [whole(packed.at[h], bra_at(ROW_JOB, inside + t)) for h in range(2)], axis=0
            ),
        )

    @pl.when(needs_row)
    def _():
        swap_row().start()

    @pl.when(first)
    def _():
        gather(wrap_out, lambda t: whole(packed.at[half], far_ket_at(WRAP_JOB, t)))
        swap_wrap().start()

    swap(0).start()
    swap(1).start()

    @pl.when(quad == 3)
    def _():
        for turn in RIGHT_ASIDE + RIGHT_OWN:
            gather(
                extra_out.at[turn],
                lambda t: whole(packed.at[1 - half], bra_at(NEXT_JOB, turn * cross + t)),
            )
        for turn in RIGHT_ASIDE:
            extra_aside(turn).start()

    @pl.when(quad == 0)
    def _():
        for turn in LEFT_ASIDE + LEFT_OWN:
            gather(
                extra_out.at[turn],
                lambda t: whole(packed.at[half], ket_at(PREV_JOB, turn * cross + t)),
            )
        for turn in LEFT_ASIDE:
            extra_aside(turn).start()

    def pass_near(cut):
        carry_left(cut).wait_recv()
        to_last(cut).start()
        carry_right(cut).wait_recv()
        to_first(cut).start()

    def relay_on(c):
        row_relayed(c).wait_recv()
        relayed(c).start()

    for cut in range(CUTS):
        hop_right(cut).wait_recv()
        on_right(cut).start()
        hop_left(cut).wait_recv()

        on_left(cut).start()

        @pl.when(first)
        def _(cut=cut):
            carry_left(cut).start()

        @pl.when(last)
        def _(cut=cut):
            carry_right(cut).start()
            if cut:
                pass_near(cut - 1)

        @pl.when((core == 1) & (place < row - 1))
        def _(cut=cut):
            for c in range(cut * CHUNKS // CUTS, (cut + 1) * CHUNKS // CUTS):
                relay_on(c)

    @pl.when(quad == 3)
    def _():
        for turn in RIGHT_OWN:
            hop_extra(turn).start()

    @pl.when(quad == 0)
    def _():
        for turn in LEFT_OWN:
            hop_extra(turn).start()

    @pl.when(beside == 3)
    def _():
        for turn in RIGHT_ASIDE:
            extra_aside(turn).wait_recv()
            extra_back(turn).start()

    @pl.when(beside == 0)
    def _():
        for turn in LEFT_ASIDE:
            extra_aside(turn).wait_recv()
            extra_back(turn).start()

    @pl.when(last)
    def _():
        pass_near(CUTS - 1)

    swap(0).wait_recv()
    total = packed_sum(
        zero,
        lambda t: whole(packed.at[1 - next_half], bra_at(NEXT_JOB, t)),
        lambda t: whole(left1, ket_at(NEXT_JOB, t)),
        inside,
    )
    total = packed_sum(
        total, lambda t: cross_in[0, t], lambda t: whole(left1, far_ket_at(NEXT_JOB, t)), cross
    )
    keep(NEXT_JOB, total)

    swap(1).wait_recv()

    @pl.when(quad != 0)
    def _():
        total = packed_sum(
            zero,
            lambda t: whole(right1, bra_at(PREV_JOB, t)),
            lambda t: whole(packed.at[half], ket_at(PREV_JOB, t)),
            inside,
        )
        total = packed_sum(
            total,
            lambda t: whole(right1, bra_at(PREV_JOB, inside + t)),
            lambda t: cross_in[1, t],
            cross,
        )
        keep(PREV_JOB, total)

    @pl.when(quad != 3)
    def _():
        result(1).start()

    def along_row():
        each(lambda c: row_direct(c).wait_recv())
        row_total[...] = whole_sum(
            jnp.zeros(row_total.shape, jnp.float32),
            lambda t: own[bra_at(ROW_JOB, t)],
            lambda t: ahead[ket_at(ROW_JOB, t)],
            inside,
        )

        @pl.when(core == 0)
        def _():
            swap_row().wait_recv()
            row_total[...] = whole_sum(
                row_total[...], lambda t: row_in[t], lambda t: ahead[far_ket_at(ROW_JOB, t)], cross
            )

        @pl.when(core == 1)
        def _():
            row_total[...] = whole_sum(
                row_total[...],
                lambda t: own[bra_at(ROW_JOB, inside + t)],
                lambda t: relay[ket_at(ROW_JOB, inside + t)],
                cross,
            )

        lower = row_total[pl.ds(bands, bands)]
        keep(
            ROW_JOB,
            row_total[pl.ds(0, bands)]
            + jnp.concatenate([lower[:, bands:], -lower[:, :bands]], axis=1),
        )
        result(0).start()

    @pl.when(core == 0)
    def _():
        along_row()

    def wrap_at_last():
        for cut in range(CUTS):
            to_last(cut).wait_recv()
        swap_row().wait_recv()
        lines = pl.ds(pl.multiple_of((1 - half) * bands, bands), bands)
        total = packed_sum(
            zero,
            lambda t: whole(packed.at[1 - half], bra_at(ROW_JOB, t)),
            lambda t: whole(near, ket_at(ROW_JOB, t)),
            inside,
        )
        total = packed_sum(
            total,
            lambda t: row_in[t, lines, :],
            lambda t: whole(near, far_ket_at(ROW_JOB, t)),
            cross,
        )
        keep(ROW_JOB, total)
        result(0).start()

    def wrap_at_first():
        for cut in range(CUTS):
            to_last(cut).wait_recv()
        swap_wrap().wait_recv()
        total = packed_sum(
            zero,
            lambda t: whole(near, bra_at(WRAP_JOB, t)),
            lambda t: whole(packed.at[half], ket_at(WRAP_JOB, t)),
            inside,
        )
        total = packed_sum(
            total,
            lambda t: whole(near, bra_at(WRAP_JOB, inside + t)),
            lambda t: wrap_in[t],
            cross,
        )
        keep(WRAP_JOB, total)
        for slot in WRAPPED:
            result(slot).start()

    def far_swaps(cut):
        on_right(cut).wait_recv()
        gather(far_out.at[0, cut], lambda t: right2[cut][bra_at(FAR_JOB, inside + t)])
        gather(far_out.at[1, cut], lambda t: right2[cut][far_ket_at(BACK_JOB, t)])
        swap_far(0, cut).start()
        swap_far(1, cut).start()

    far_swaps(0)

    @pl.when(quad != 0)
    def _():
        result(2).start()
        result(3).start()

    for cut in range(1, CUTS):
        if cut == CUTS - 1:
            @pl.when((core == 1) & (place > 1) & (place < row - 1))
            def _():
                along_row()

            @pl.when(last)
            def _():
                wrap_at_last()

            @pl.when(first)
            def _():
                wrap_at_first()

        far_swaps(cut)

    def previous_extra():
        def source(turn):
            if turn * cross < inside:
                ket = lambda t: whole(packed.at[half], ket_at(PREV_JOB, turn * cross + t))
            else:
                ket = lambda t: cross_in[1, t]
            return lambda t: extra[turn, t], ket

        totals = (zero, zero)
        for turns in zip(RIGHT_OWN, RIGHT_ASIDE):
            for turn in turns:
                hop_extra(turn).wait_recv()
            totals = packed_sums(totals, [source(turn) for turn in turns], cross)
        keep(PREV_JOB, totals[0] + totals[1])
        result(2).start()
        result(3).start()

    for cut in range(CUTS):
        on_left(cut).wait_recv()
    far, back = packed_sums(
        (zero, zero),
        (
            (lambda t: whole_far(bra_at(FAR_JOB, t)), lambda t: whole(left2, ket_at(FAR_JOB, t))),
            (lambda t: whole(left2, bra_at(BACK_JOB, t)), lambda t: whole_far(ket_at(BACK_JOB, t))),
        ),
        inside,
    )

    @pl.when(place == 1)
    def _():
        along_row()

    for cut in range(CUTS):
        swap_far(0, cut).wait_recv()
        swap_far(1, cut).wait_recv()
    far, back = packed_sums(
        (far, back),
        (
            (
                lambda t: whole(far_in.at[0], t),
                lambda t: whole(left2, far_ket_at(FAR_JOB, t)),
            ),
            (
                lambda t: whole(left2, bra_at(BACK_JOB, inside + t)),
                lambda t: whole(far_in.at[1], t),
            ),
        ),
        cross,
    )
    keep(FAR_JOB, far)
    keep(BACK_JOB, back)
    for slot in (4, 5, 6, 7):
        result(slot).start()

    @pl.when(quad == 0)
    def _():
        previous_extra()

    @pl.when(quad == 3)
    def _():
        for turn in LEFT:
            hop_extra(turn).wait_recv()

        def source(turn):
            return (
                lambda t: whole(packed.at[1 - half], bra_at(NEXT_JOB, turn * cross + t)),
                lambda t: extra[turn, t],
            )

        more = packed_sums((zero, zero), [source(turn) for turn in LEFT], cross)
        keep(NEXT_JOB, parts[NEXT_JOB].reshape(zero.shape) + (more[0] + more[1]))
        result(1).start()

    for slot in range(WRAPPED[0]):
        result(slot).wait_recv()
    inbox[0] = inbox[0] + parts[ROW_JOB, ga]

    @pl.when(last)
    def _():
        for slot in WRAPPED:
            result(slot).wait_recv()
        inbox[0] = inbox[0] + (inbox[8] + inbox[9])

    found = [
        inbox[0],
        (parts[NEXT_JOB, ga] + inbox[1]) + (inbox[2] + inbox[3]),
        (inbox[4] + inbox[5]) + (inbox[6] + inbox[7]),
    ]
    for b in range(columns):
        target = jnp.broadcast_to(neighbour[:, b : b + 1], found[0].shape)
        chosen = jnp.where(
            target == at(steps[0]), found[0], jnp.where(target == at(steps[1]), found[1], found[2])
        )
        out[b, 0] = chosen[:, :bands]
        out[b, 1] = chosen[:, bands:]

    def drain(c):
        @pl.when(place > 0)
        def _():
            row_direct(c).wait_send()

        @pl.when((core == 1) & (place < row - 1))
        def _():
            relayed(c).wait_send()

    each(drain)
    for cut in range(CUTS):
        hop_right(cut).wait_send()
        hop_left(cut).wait_send()
        on_right(cut).wait_send()
        on_left(cut).wait_send()
        swap_far(0, cut).wait_send()
        swap_far(1, cut).wait_send()
    for i in range(4):
        send_shift(i).wait_send()

    @pl.when(quad == 3)
    def _():
        for turn in RIGHT:
            hop_extra(turn).wait_send()

    @pl.when(quad == 0)
    def _():
        for turn in LEFT:
            hop_extra(turn).wait_send()

    @pl.when(beside == 3)
    def _():
        for turn in RIGHT_ASIDE:
            extra_back(turn).wait_send()

    @pl.when(beside == 0)
    def _():
        for turn in LEFT_ASIDE:
            extra_back(turn).wait_send()

    @pl.when(first)
    def _():
        swap_wrap().wait_send()
        for cut in range(CUTS):
            carry_left(cut).wait_send()
        for slot in WRAPPED:
            result(slot).wait_send()

    @pl.when(last)
    def _():
        for cut in range(CUTS):
            carry_right(cut).wait_send()
            to_last(cut).wait_send()
            to_first(cut).wait_send()

    @pl.when(needs_row)
    def _():
        swap_row().wait_send()

    for i in range(2):
        swap(i).wait_send()
    for slot in range(WRAPPED[0]):
        result(slot).wait_send()


def on_device(coeffs, neighbour, shift_id, block_map):
    _, blocks, _, bands, lanes = coeffs.shape
    columns = neighbour.shape[1]
    n_ka = lax.axis_size("ka")
    row = n_ka // 8
    cross = 2 * max(1, blocks // 12)
    def half_buffer(*lead):
        return pltpu.VMEM((*lead, bands, lanes), jnp.bfloat16)

    def cut_buffer(*lead):
        return pltpu.VMEM((*lead, bands // CUTS, lanes), jnp.bfloat16)

    def whole_buffer(*lead):
        return pltpu.VMEM((*lead, 2 * bands, lanes), jnp.bfloat16)

    found = pl.pallas_call(
        functools.partial(kernel, n_ka, row, cross),
        out_shape=jax.ShapeDtypeStruct((columns, 2, bands // 2, bands), jnp.float32),
        in_specs=[
            pl.BlockSpec(memory_space=pl.ANY),
            pl.BlockSpec(memory_space=pl.ANY),
            pl.BlockSpec(memory_space=pl.ANY),
            pl.BlockSpec(memory_space=pl.ANY),
        ],
        out_specs=pl.BlockSpec(memory_space=pltpu.VMEM),
        scratch_shapes=[
            pltpu.VMEM(neighbour.shape, jnp.int32),
            pltpu.VMEM(shift_id.shape, jnp.int32),
            pltpu.VMEM(block_map.shape, jnp.int32),
            pltpu.VMEM((3, 8, lanes), jnp.int32),
            pltpu.VMEM((4, 8, lanes), jnp.int32),
            pltpu.VMEM((24, lanes), jnp.int32),
            pltpu.SMEM((24, lanes), jnp.int32),
            whole_buffer(blocks),
            cut_buffer(2, CUTS, blocks),
            cut_buffer(CUTS, blocks),
            *[cut_buffer(blocks) for _ in range(CUTS)],
            cut_buffer(CUTS, blocks), cut_buffer(CUTS, blocks),
            half_buffer(TURNS, cross), half_buffer(TURNS, cross), half_buffer(TURNS, cross),
            whole_buffer(blocks), whole_buffer(blocks),
            cut_buffer(CUTS, blocks), cut_buffer(CUTS, blocks), cut_buffer(CUTS, blocks),
            half_buffer(cross), half_buffer(cross),
            whole_buffer(cross), whole_buffer(cross),
            half_buffer(2, cross), half_buffer(2, cross),
            cut_buffer(2, CUTS, cross), cut_buffer(2, CUTS, cross),
            pltpu.VMEM((2 * bands, 2 * bands), jnp.float32),
            pltpu.VMEM((JOBS, 2, bands // 2, 2 * bands), jnp.float32),
            pltpu.VMEM((10, bands // 2, 2 * bands), jnp.float32),
            pltpu.SemaphoreType.DMA((3,)),
            pltpu.SemaphoreType.DMA((5, CHUNKS)),
            pltpu.SemaphoreType.DMA((8, CUTS)),
            pltpu.SemaphoreType.DMA((2, 4)),
            pltpu.SemaphoreType.DMA,
            pltpu.SemaphoreType.DMA((7, CUTS)),
            pltpu.SemaphoreType.DMA((2,)),
            pltpu.SemaphoreType.DMA((4, TURNS)),
            pltpu.SemaphoreType.DMA((2,)),
            pltpu.SemaphoreType.DMA((2, 2)),
            pltpu.SemaphoreType.DMA((2, 2, CUTS)),
            pltpu.SemaphoreType.DMA((2, 10)),
        ],
        compiler_params=pltpu.CompilerParams(
            collective_id=0, has_side_effects=True, vmem_limit_bytes=61 * 2**20
        ),
        name="overlaps",
    )(neighbour, shift_id, block_map, coeffs.reshape(blocks, 2 * bands, lanes))
    return found[None]


def solution(mesh):
    in_specs = (P("ka", "ga", None, None, None), P("ka", None), P("ka", None), P())
    out_specs = P("ka", None, None, "ga", None)
    return jax.shard_map(
        on_device, mesh=mesh, in_specs=in_specs, out_specs=out_specs, check_vma=False
    )
```

```python
import functools

import jax
import jax.numpy as jnp
from jax import lax
from jax.experimental import pallas as pl
from jax.experimental.pallas import tpu as pltpu
from jax.sharding import PartitionSpec as P

MESH = pl.DeviceIdType.MESH
CHUNKS = 8
CUTS = 4
TURNS = 12
LEFT_OWN, LEFT_ASIDE = (0, 1, 2), (3, 4, 5)
RIGHT_OWN, RIGHT_ASIDE = (6, 7, 8), (9, 10, 11)
LEFT = LEFT_OWN + LEFT_ASIDE
RIGHT = RIGHT_OWN + RIGHT_ASIDE
PACK = 5
STEP = 20
CONTRACT = (((1,), (1,)), ((), ()))

LOAD, ROW_SENT, RELAY_IN, RELAY_SENT, ROW_IN = range(5)
RIGHT1_SENT, RIGHT1_IN, RIGHT2_SENT, RIGHT2_IN = range(4)
LEFT1_SENT, LEFT1_IN, LEFT2_SENT, LEFT2_IN = range(4, 8)
ROW_JOB, NEXT_JOB, PREV_JOB, FAR_JOB, BACK_JOB, WRAP_JOB = range(6)
JOBS = 6


def flipped(block):
    half = block.shape[1] // 2
    return jnp.concatenate([block[:, half:], -block[:, :half]], axis=1)


def kernel(
    n_ka, row, cross, neighbour_in, shift_in, map_in, coeffs, out,
    neighbour, shift_id, block_map,    shifts_out, shifts_in, table_rows, table, own, packed, right1, right2_0, right2_1, right2_2, right2_3, left1, left2,
    extra, extra_out, extra_via, relay, ahead, near, pass_a, pass_b, wrap_out, wrap_in,
    row_out, row_in, cross_out, cross_in, far_out, far_in, row_total, parts, inbox,
    small_sem, chunk_sem, hop_sem, shift_sem, table_sem, near_sem, wrap_sem, extra_sem, row_cross_sem, cross_sem,
    far_sem, result_sem,
):
    blocks = own.shape[0]
    bands = own.shape[1] // 2
    lanes = own.shape[2]
    deep = bands // CUTS
    right2 = (right2_0, right2_1, right2_2, right2_3)
    size = blocks // CHUNKS
    inside = blocks - cross
    turn_size = blocks // TURNS
    ka = lax.axis_index("ka")
    ga = lax.axis_index("ga")
    other = 1 - ga
    core = lax.rem(ka, 2)
    place = lax.rem(ka, row)
    odd = lax.rem(place // 4, 2)
    aside = 4 - 8 * odd
    turned = jnp.where(odd == 1, 3 - 2 * core, 2 * core)
    plane = lax.rem(ka // row + turned, 8)
    beside = lax.rem(ka // row + 3 - turned, 4)
    first = place == 0
    last = place == row - 1
    quad = lax.rem(plane, 4)
    half = plane // 4
    needs_row = (core == 0) | last
    next_half = lax.rem(plane + 1, 8) // 4

    def at(step):
        return lax.rem(ka + n_ka + step, n_ka)

    def part(c):
        return pl.ds(c * size, size)

    def remote(source, target, sent, arrived, device):
        return pltpu.make_async_remote_copy(
            src_ref=source, dst_ref=target, send_sem=sent, recv_sem=arrived,
            device_id=device, device_id_type=MESH,
        )

    def load(i):
        lines = pl.ds((i // 2 + lax.rem(i, 2) * CUTS) * deep, deep)
        return pltpu.make_async_copy(
            coeffs.at[:, lines], own.at[:, lines], chunk_sem.at[LOAD, i]
        )

    def row_direct(c):
        return remote(
            own.at[part(c)], ahead.at[part(c)],
            chunk_sem.at[ROW_SENT, c], chunk_sem.at[ROW_IN, c], (at(-1), ga),
        )

    def row_relayed(c):
        return remote(
            own.at[part(c)], relay.at[part(c)],
            chunk_sem.at[ROW_SENT, c], chunk_sem.at[RELAY_IN, c], (at(-1), other),
        )

    def relayed(c):
        return remote(
            relay.at[part(c)], ahead.at[part(c)],
            chunk_sem.at[RELAY_SENT, c], chunk_sem.at[ROW_IN, c], (ka, other),
        )

    def hop(source, target, sent, cut, step):
        return remote(
            source, target, hop_sem.at[sent, cut], hop_sem.at[sent + 1, cut], (at(step * row), ga)
        )

    def hop_right(cut):
        return hop(packed.at[half, cut], right1.at[cut], RIGHT1_SENT, cut, 1)

    def hop_left(cut):
        return hop(packed.at[1 - half, cut], left1.at[cut], LEFT1_SENT, cut, -1)

    def on_right(cut):
        return hop(right1.at[cut], right2[cut], RIGHT2_SENT, cut, 1)

    def on_left(cut):
        return hop(left1.at[cut], left2.at[cut], LEFT2_SENT, cut, -1)

    def hop_extra(turn):
        return remote(
            extra_out.at[turn], extra.at[turn],
            extra_sem.at[0, turn], extra_sem.at[1, turn],
            (at(-row if turn in LEFT else row), ga),
        )

    def extra_aside(turn):
        return remote(
            extra_out.at[turn], extra_via.at[turn],
            extra_sem.at[0, turn], extra_sem.at[2, turn], (at(aside), ga),
        )

    def extra_back(turn):
        return remote(
            extra_via.at[turn], extra.at[turn],
            extra_sem.at[3, turn], extra_sem.at[1, turn],
            (at(aside + (-row if turn in LEFT else row)), ga),
        )

    def carry_left(cut):
        return remote(
            left1.at[cut], pass_a.at[cut],
            near_sem.at[0, cut], near_sem.at[1, cut], (at(row - 1), other),
        )

    def carry_right(cut):
        return remote(
            right1.at[cut], pass_b.at[cut],
            near_sem.at[2, cut], near_sem.at[3, cut], (ka, other),
        )

    def to_last(cut):
        return remote(
            pass_a.at[cut], near.at[cut], near_sem.at[4, cut], near_sem.at[5, cut], (ka, other)
        )

    def to_first(cut):
        return remote(
            pass_b.at[cut], near.at[cut],
            near_sem.at[6, cut], near_sem.at[5, cut], (at(1 - row), other),
        )

    def swap_wrap():
        return remote(wrap_out, wrap_in, wrap_sem.at[0], wrap_sem.at[1], (ka, other))

    def swap_row():
        return remote(row_out, row_in, row_cross_sem.at[0], row_cross_sem.at[1], (ka, other))

    def swap(i):
        return remote(
            cross_out.at[i], cross_in.at[i], cross_sem.at[0, i], cross_sem.at[1, i], (ka, other)
        )

    def swap_far(i, cut):
        return remote(
            far_out.at[i, cut], far_in.at[i, cut],
            far_sem.at[0, i, cut], far_sem.at[1, i, cut], (ka, other),
        )

    def result(slot):
        job, step, same = RESULTS[slot]
        side = ga if same else other
        return remote(
            parts.at[job, side], inbox.at[slot],
            result_sem.at[0, slot], result_sem.at[1, slot], (at(step), side),
        )

    RESULTS = (
        (ROW_JOB, 0, False), (NEXT_JOB, 0, False),
        (PREV_JOB, -row, True), (PREV_JOB, -row, False),
        (FAR_JOB, -2 * row, True), (FAR_JOB, -2 * row, False),
        (BACK_JOB, 2 * row, True), (BACK_JOB, 2 * row, False),
        (WRAP_JOB, -1, True), (WRAP_JOB, -1, False),
    )
    WRAPPED = (8, 9)

    def each(body):
        def run(c, carry):
            body(c)
            return carry
        lax.fori_loop(0, CHUNKS, run, 0)

    def bra_at(job, t):
        return table[job, t]

    def ket_at(job, t):
        return table[JOBS + job, t]

    def far_ket_at(job, t):
        return table[2 * JOBS + job, inside + t]

    def whole(source, index):
        return jnp.concatenate([source[cut, index] for cut in range(CUTS)], axis=0)

    def whole_far(index):
        return jnp.concatenate([right2[cut][index] for cut in range(CUTS)], axis=0)

    def gather(target, pick, count=cross):
        def run(t, carry):
            for u in range(PACK):
                target[t * PACK + u] = pick(t * PACK + u)
            return carry
        lax.fori_loop(0, count // PACK, run, 0)

    def whole_sum(total, bra, ket, count):
        def run(s, total):
            left = jnp.concatenate([bra(s * STEP + u) for u in range(STEP)], axis=1)
            right = jnp.concatenate([ket(s * STEP + u) for u in range(STEP)], axis=1)
            return total + lax.dot_general(
                left, right, CONTRACT, preferred_element_type=jnp.float32
            )
        return lax.fori_loop(0, count // STEP, run, total)

    def packed_step(total, pairs):
        left = jnp.concatenate([bra for bra, _ in pairs], axis=1)
        right = jnp.concatenate(
            [jnp.concatenate([ket for _, ket in pairs], axis=1),
             jnp.concatenate([flipped(ket) for _, ket in pairs], axis=1)], axis=0
        )
        return total + lax.dot_general(
            left, right, CONTRACT, preferred_element_type=jnp.float32
        )

    def packed_sums(totals, sources, count, width=STEP):
        def run(s, totals):
            return tuple(
                packed_step(
                    total, [(bra(s * width + u), ket(s * width + u)) for u in range(width)]
                )
                for total, (bra, ket) in zip(totals, sources)
            )
        return lax.fori_loop(0, count // width, run, tuple(totals))

    def packed_sum(total, bra, ket, count):
        return packed_sums((total,), ((bra, ket),), count)[0]

    def keep(job, total):
        parts[job] = total.reshape(parts.shape[1:])

    zero = jnp.zeros((bands, 2 * bands), jnp.float32)

    barrier = pltpu.get_barrier_semaphore()
    meet = [
        (ka, other), (at(row), ga), (at(-row), ga), (at(row), other), (at(-row), other),
        (at(2 * row), ga), (at(-2 * row), ga), (at(2 * row), other), (at(-2 * row), other),
        (at(-1), ga), (at(1), ga), (at(-1), other), (at(1), other),
        (at(aside), ga), (at(aside + row), ga), (at(aside - row), ga),
    ]
    def greet(device):
        pl.semaphore_signal(barrier, inc=1, device_id=device, device_id_type=MESH)

    for device in meet:
        greet(device)

    @pl.when(first)
    def _():
        greet((at(row - 1), other))

    @pl.when(last)
    def _():
        greet((at(1 - row), other))

    small = [
        pltpu.make_async_copy(given, held, small_sem.at[i])
        for i, (given, held) in enumerate(
            ((neighbour_in, neighbour), (shift_in, shift_id), (map_in, block_map))
        )
    ]
    for copy in small:
        copy.start()
    each(lambda c: load(c).start())
    for copy in small:
        copy.wait()

    tile = (8, lanes)
    columns = neighbour.shape[1]
    targets = [jnp.broadcast_to(neighbour[:, b : b + 1], tile) for b in range(columns)]
    steps = (1, row, n_ka // 2)

    def shift_of(step):
        found = jnp.zeros(tile, jnp.int32)
        for b in range(columns):
            moved = jnp.broadcast_to(shift_id[:, b : b + 1], tile)
            found = found + jnp.where(targets[b] == at(step), moved, 0)
        return found

    row_shift, next_shift, far_shift = [shift_of(step) for step in steps]
    shifts_out[0] = next_shift
    shifts_out[1] = far_shift
    shifts_out[2] = row_shift

    def send_shift(i):
        return remote(
            shifts_out.at[(0, 1, 1, 2)[i]], shifts_in.at[i],
            shift_sem.at[0, i], shift_sem.at[1, i], (at((row, 2 * row, -2 * row, 1)[i]), ga),
        )

    def load_cut(cut):
        load(2 * cut).wait()
        load(2 * cut + 1).wait()

    def pack_cut(cut):
        def pack(t, carry):
            for u in range(STEP):
                j = t * STEP + u
                real = own[j, pl.ds(cut * deep, deep), :]
                imag = own[j, pl.ds(bands + cut * deep, deep), :]
                mid = lanes // 2
                packed[0, cut, j] = jnp.concatenate([real[:, :mid], imag[:, :mid]], axis=1)
                packed[1, cut, j] = jnp.concatenate([real[:, mid:], imag[:, mid:]], axis=1)
            return carry
        lax.fori_loop(0, blocks // STEP, pack, 0)

    load_cut(0)
    pack_cut(0)
    pl.semaphore_wait(barrier, len(meet) + jnp.where(first | last, 1, 0))
    for i in range(4):
        send_shift(i).start()

    def make_table():
        lane = lax.broadcasted_iota(jnp.int32, (lanes, lanes), 1)
        line = lax.broadcasted_iota(jnp.int32, (lanes, lanes), 0)
        maps = [
            jnp.concatenate(
                [block_map[:, a * blocks : (a + 1) * blocks],
                 jnp.zeros((block_map.shape[0], lanes - blocks), jnp.int32)], axis=1
            )
            for a in range(2)
        ]
        maps = [jnp.where(ga == a, maps[0], maps[1]) for a in range(2)]
        shifts = [row_shift, next_shift] + [shifts_in[i] for i in range(4)]
        choice = lax.broadcasted_iota(jnp.int32, tile, 0)
        rows = [
            jnp.sum(jnp.where(shift == choice, each_map, 0), axis=0, keepdims=True)
            for each_map in maps for shift in shifts
        ]
        rows = jnp.concatenate(rows + [jnp.zeros((16 - 2 * JOBS, lanes), jnp.int32)], axis=0)
        number = lax.broadcasted_iota(jnp.int32, rows.shape, 0)
        spot = lax.broadcasted_iota(jnp.int32, rows.shape, 1)
        source = jnp.where(rows >= blocks, 1, 0)
        same = jnp.where(source == jnp.where(number < JOBS, ga, other), 1, 0)
        local = rows - blocks * source
        same_t = same.T
        kept = [
            jnp.sum(jnp.where(line < lane, same_t[:, r : r + 1], 0), axis=0, keepdims=True)
            for r in range(2 * JOBS)
        ]
        kept = jnp.concatenate(kept + [jnp.zeros((16 - 2 * JOBS, lanes), jnp.int32)], axis=0)
        rank = jnp.where(same == 1, kept, inside + spot - kept)
        rank_t = jnp.where(spot < blocks, rank, -1).T
        local_t = local.T
        hits = [rank_t[:, r : r + 1] == lane for r in range(2 * JOBS)]
        lists = [jnp.sum(jnp.where(hits[r], line, 0), axis=0, keepdims=True) for r in range(JOBS)]
        lists += [
            jnp.sum(jnp.where(hits[r], local_t[:, r : r + 1], 0), axis=0, keepdims=True)
            for r in range(2 * JOBS)
        ]
        lists += [jnp.zeros((24 - 3 * JOBS, lanes), jnp.int32)]
        table_rows[...] = jnp.concatenate(lists, axis=0)

    def first_sends(c):
        @pl.when(core == 1)
        def _():
            row_direct(c).start()

        @pl.when((core == 0) & (place > 0))
        def _():
            row_relayed(c).start()

    hop_right(0).start()
    hop_left(0).start()
    for cut in range(1, CUTS):
        load_cut(cut)
    each(first_sends)
    pack_cut(1)
    for cut in range(1, CUTS):
        if cut + 1 < CUTS:
            pack_cut(cut + 1)
        hop_right(cut).start()
        hop_left(cut).start()
    for i in range(4):
        send_shift(i).wait_recv()
    make_table()
    fetch = pltpu.make_async_copy(table_rows, table, table_sem)
    fetch.start()
    fetch.wait()
    gather(cross_out.at[0], lambda t: whole(packed.at[1 - next_half], bra_at(NEXT_JOB, inside + t)))
    gather(cross_out.at[1], lambda t: whole(packed.at[half], far_ket_at(PREV_JOB, t)))

    @pl.when(core == 0)
    def _():
        gather(row_out, lambda t: own[bra_at(ROW_JOB, inside + t)])

    @pl.when(last)
    def _():
        gather(
            row_out,
            lambda t: jnp.concatenate(
                [whole(packed.at[h], bra_at(ROW_JOB, inside + t)) for h in range(2)], axis=0
            ),
        )

    @pl.when(needs_row)
    def _():
        swap_row().start()

    @pl.when(first)
    def _():
        gather(wrap_out, lambda t: whole(packed.at[half], far_ket_at(WRAP_JOB, t)))
        swap_wrap().start()

    swap(0).start()
    swap(1).start()

    @pl.when(quad == 3)
    def _():
        for turn in RIGHT_ASIDE + RIGHT_OWN:
            gather(
                extra_out.at[turn],
                lambda t: whole(packed.at[1 - half], bra_at(NEXT_JOB, turn * turn_size + t)),
                turn_size,
            )
        for turn in RIGHT_ASIDE:
            extra_aside(turn).start()

    @pl.when(quad == 0)
    def _():
        for turn in LEFT_ASIDE + LEFT_OWN:
            gather(
                extra_out.at[turn],
                lambda t: whole(packed.at[half], ket_at(PREV_JOB, turn * turn_size + t)),
                turn_size,
            )
        for turn in LEFT_ASIDE:
            extra_aside(turn).start()

    def pass_near(cut):
        carry_left(cut).wait_recv()
        to_last(cut).start()
        carry_right(cut).wait_recv()
        to_first(cut).start()

    def relay_on(c):
        row_relayed(c).wait_recv()
        relayed(c).start()

    for cut in range(CUTS):
        hop_right(cut).wait_recv()
        on_right(cut).start()
        hop_left(cut).wait_recv()

        on_left(cut).start()

        @pl.when(first)
        def _(cut=cut):
            carry_left(cut).start()

        @pl.when(last)
        def _(cut=cut):
            carry_right(cut).start()
            if cut:
                pass_near(cut - 1)

        @pl.when((core == 1) & (place < row - 1))
        def _(cut=cut):
            for c in range(cut * CHUNKS // CUTS, (cut + 1) * CHUNKS // CUTS):
                relay_on(c)

    @pl.when(quad == 3)
    def _():
        for turn in RIGHT_OWN:
            hop_extra(turn).start()

    @pl.when(quad == 0)
    def _():
        for turn in LEFT_OWN:
            hop_extra(turn).start()

    @pl.when(beside == 3)
    def _():
        for turn in RIGHT_ASIDE:
            extra_aside(turn).wait_recv()
            extra_back(turn).start()

    @pl.when(beside == 0)
    def _():
        for turn in LEFT_ASIDE:
            extra_aside(turn).wait_recv()
            extra_back(turn).start()

    @pl.when(last)
    def _():
        pass_near(CUTS - 1)

    swap(0).wait_recv()
    total = packed_sum(
        zero,
        lambda t: whole(packed.at[1 - next_half], bra_at(NEXT_JOB, t)),
        lambda t: whole(left1, ket_at(NEXT_JOB, t)),
        inside,
    )
    total = packed_sum(
        total, lambda t: cross_in[0, t], lambda t: whole(left1, far_ket_at(NEXT_JOB, t)), cross
    )
    keep(NEXT_JOB, total)

    swap(1).wait_recv()

    @pl.when(quad != 0)
    def _():
        total = packed_sum(
            zero,
            lambda t: whole(right1, bra_at(PREV_JOB, t)),
            lambda t: whole(packed.at[half], ket_at(PREV_JOB, t)),
            inside,
        )
        total = packed_sum(
            total,
            lambda t: whole(right1, bra_at(PREV_JOB, inside + t)),
            lambda t: cross_in[1, t],
            cross,
        )
        keep(PREV_JOB, total)

    @pl.when(quad != 3)
    def _():
        result(1).start()

    def along_row():
        each(lambda c: row_direct(c).wait_recv())
        row_total[...] = whole_sum(
            jnp.zeros(row_total.shape, jnp.float32),
            lambda t: own[bra_at(ROW_JOB, t)],
            lambda t: ahead[ket_at(ROW_JOB, t)],
            inside,
        )

        @pl.when(core == 0)
        def _():
            swap_row().wait_recv()
            row_total[...] = whole_sum(
                row_total[...], lambda t: row_in[t], lambda t: ahead[far_ket_at(ROW_JOB, t)], cross
            )

        @pl.when(core == 1)
        def _():
            row_total[...] = whole_sum(
                row_total[...],
                lambda t: own[bra_at(ROW_JOB, inside + t)],
                lambda t: relay[ket_at(ROW_JOB, inside + t)],
                cross,
            )

        lower = row_total[pl.ds(bands, bands)]
        keep(
            ROW_JOB,
            row_total[pl.ds(0, bands)]
            + jnp.concatenate([lower[:, bands:], -lower[:, :bands]], axis=1),
        )
        result(0).start()

    @pl.when(core == 0)
    def _():
        along_row()

    def wrap_at_last():
        for cut in range(CUTS):
            to_last(cut).wait_recv()
        swap_row().wait_recv()
        lines = pl.ds(pl.multiple_of((1 - half) * bands, bands), bands)
        total = packed_sum(
            zero,
            lambda t: whole(packed.at[1 - half], bra_at(ROW_JOB, t)),
            lambda t: whole(near, ket_at(ROW_JOB, t)),
            inside,
        )
        total = packed_sum(
            total,
            lambda t: row_in[t, lines, :],
            lambda t: whole(near, far_ket_at(ROW_JOB, t)),
            cross,
        )
        keep(ROW_JOB, total)
        result(0).start()

    def wrap_at_first():
        for cut in range(CUTS):
            to_last(cut).wait_recv()
        swap_wrap().wait_recv()
        total = packed_sum(
            zero,
            lambda t: whole(near, bra_at(WRAP_JOB, t)),
            lambda t: whole(packed.at[half], ket_at(WRAP_JOB, t)),
            inside,
        )
        total = packed_sum(
            total,
            lambda t: whole(near, bra_at(WRAP_JOB, inside + t)),
            lambda t: wrap_in[t],
            cross,
        )
        keep(WRAP_JOB, total)
        for slot in WRAPPED:
            result(slot).start()

    def far_swaps(cut):
        on_right(cut).wait_recv()
        gather(far_out.at[0, cut], lambda t: right2[cut][bra_at(FAR_JOB, inside + t)])
        gather(far_out.at[1, cut], lambda t: right2[cut][far_ket_at(BACK_JOB, t)])
        swap_far(0, cut).start()
        swap_far(1, cut).start()

    far_swaps(0)

    @pl.when(quad != 0)
    def _():
        result(2).start()
        result(3).start()

    for cut in range(1, CUTS):
        if cut == CUTS - 1:
            @pl.when((core == 1) & (place < row - 1))
            def _():
                along_row()

            @pl.when(last)
            def _():
                wrap_at_last()

            @pl.when(first)
            def _():
                wrap_at_first()

        far_swaps(cut)

    def previous_extra(turn):
        if turn * turn_size < inside:
            ket = lambda t: whole(packed.at[half], ket_at(PREV_JOB, turn * turn_size + t))
        else:
            ket = lambda t: cross_in[1, turn * turn_size - inside + t]
        return lambda t: extra[turn, t], ket

    def next_extra(turn):
        return (
            lambda t: whole(packed.at[1 - half], bra_at(NEXT_JOB, turn * turn_size + t)),
            lambda t: extra[turn, t],
        )

    def extra_sum(turns, source):
        totals = (zero, zero)
        for pair in turns:
            for turn in pair:
                hop_extra(turn).wait_recv()
            totals = packed_sums(totals, [source(turn) for turn in pair], turn_size, turn_size)
        return totals[0] + totals[1]

    def kept(job):
        return parts[job].reshape(zero.shape)

    from_left = tuple(zip(RIGHT_OWN, RIGHT_ASIDE))
    from_right = tuple(zip(LEFT_OWN, LEFT_ASIDE))

    for cut in range(CUTS):
        on_left(cut).wait_recv()
    far, back = packed_sums(
        (zero, zero),
        (
            (lambda t: whole_far(bra_at(FAR_JOB, t)), lambda t: whole(left2, ket_at(FAR_JOB, t))),
            (lambda t: whole(left2, bra_at(BACK_JOB, t)), lambda t: whole_far(ket_at(BACK_JOB, t))),
        ),
        inside,
    )

    @pl.when(quad == 0)
    def _():
        keep(PREV_JOB, extra_sum(from_left[:2], previous_extra))

    @pl.when(quad == 3)
    def _():
        keep(NEXT_JOB, kept(NEXT_JOB) + extra_sum(from_right[:2], next_extra))

    for cut in range(CUTS):
        swap_far(0, cut).wait_recv()
        swap_far(1, cut).wait_recv()
    far, back = packed_sums(
        (far, back),
        (
            (
                lambda t: whole(far_in.at[0], t),
                lambda t: whole(left2, far_ket_at(FAR_JOB, t)),
            ),
            (
                lambda t: whole(left2, bra_at(BACK_JOB, inside + t)),
                lambda t: whole(far_in.at[1], t),
            ),
        ),
        cross,
    )
    keep(FAR_JOB, far)
    keep(BACK_JOB, back)
    for slot in (4, 5, 6, 7):
        result(slot).start()

    @pl.when(quad == 0)
    def _():
        keep(PREV_JOB, kept(PREV_JOB) + extra_sum(from_left[2:], previous_extra))
        result(2).start()
        result(3).start()

    @pl.when(quad == 3)
    def _():
        keep(NEXT_JOB, kept(NEXT_JOB) + extra_sum(from_right[2:], next_extra))
        result(1).start()

    def drain(c):
        @pl.when(place > 0)
        def _():
            row_direct(c).wait_send()

        @pl.when((core == 1) & (place < row - 1))
        def _():
            relayed(c).wait_send()

    each(drain)
    for cut in range(CUTS):
        hop_right(cut).wait_send()
        hop_left(cut).wait_send()
        on_right(cut).wait_send()
        on_left(cut).wait_send()
        swap_far(0, cut).wait_send()
        swap_far(1, cut).wait_send()
    for i in range(4):
        send_shift(i).wait_send()

    @pl.when(quad == 3)
    def _():
        for turn in RIGHT:
            hop_extra(turn).wait_send()

    @pl.when(quad == 0)
    def _():
        for turn in LEFT:
            hop_extra(turn).wait_send()

    @pl.when(beside == 3)
    def _():
        for turn in RIGHT_ASIDE:
            extra_back(turn).wait_send()

    @pl.when(beside == 0)
    def _():
        for turn in LEFT_ASIDE:
            extra_back(turn).wait_send()

    @pl.when(first)
    def _():
        swap_wrap().wait_send()
        for cut in range(CUTS):
            carry_left(cut).wait_send()

    @pl.when(last)
    def _():
        for cut in range(CUTS):
            carry_right(cut).wait_send()
            to_last(cut).wait_send()
            to_first(cut).wait_send()

    @pl.when(needs_row)
    def _():
        swap_row().wait_send()

    for i in range(2):
        swap(i).wait_send()
    for slot in range(WRAPPED[0]):
        result(slot).wait_recv()
    inbox[0] = inbox[0] + parts[ROW_JOB, ga]

    @pl.when(last)
    def _():
        for slot in WRAPPED:
            result(slot).wait_recv()
        inbox[0] = inbox[0] + (inbox[8] + inbox[9])

    found = [
        inbox[0],
        (parts[NEXT_JOB, ga] + inbox[1]) + (inbox[2] + inbox[3]),
        (inbox[4] + inbox[5]) + (inbox[6] + inbox[7]),
    ]
    for b in range(columns):
        target = jnp.broadcast_to(neighbour[:, b : b + 1], found[0].shape)
        chosen = jnp.where(
            target == at(steps[0]), found[0], jnp.where(target == at(steps[1]), found[1], found[2])
        )
        out[b, 0] = chosen[:, :bands]
        out[b, 1] = chosen[:, bands:]

    for slot in range(WRAPPED[0]):
        result(slot).wait_send()

    @pl.when(first)
    def _():
        for slot in WRAPPED:
            result(slot).wait_send()


def on_device(coeffs, neighbour, shift_id, block_map):
    _, blocks, _, bands, lanes = coeffs.shape
    columns = neighbour.shape[1]
    n_ka = lax.axis_size("ka")
    row = n_ka // 8
    cross = 2 * max(1, blocks // 12)
    def half_buffer(*lead):
        return pltpu.VMEM((*lead, bands, lanes), jnp.bfloat16)

    def cut_buffer(*lead):
        return pltpu.VMEM((*lead, bands // CUTS, lanes), jnp.bfloat16)

    def whole_buffer(*lead):
        return pltpu.VMEM((*lead, 2 * bands, lanes), jnp.bfloat16)

    found = pl.pallas_call(
        functools.partial(kernel, n_ka, row, cross),
        out_shape=pltpu.VMEM((columns, 2, bands // 2, bands), jnp.float32),
        in_specs=[
            pl.BlockSpec(memory_space=pl.ANY),
            pl.BlockSpec(memory_space=pl.ANY),
            pl.BlockSpec(memory_space=pl.ANY),
            pl.BlockSpec(memory_space=pl.ANY),
        ],
        out_specs=pl.BlockSpec(memory_space=pltpu.VMEM),
        scratch_shapes=[
            pltpu.VMEM(neighbour.shape, jnp.int32),
            pltpu.VMEM(shift_id.shape, jnp.int32),
            pltpu.VMEM(block_map.shape, jnp.int32),
            pltpu.VMEM((3, 8, lanes), jnp.int32),
            pltpu.VMEM((4, 8, lanes), jnp.int32),
            pltpu.VMEM((24, lanes), jnp.int32),
            pltpu.SMEM((24, lanes), jnp.int32),
            whole_buffer(blocks),
            cut_buffer(2, CUTS, blocks),
            cut_buffer(CUTS, blocks),
            *[cut_buffer(blocks) for _ in range(CUTS)],
            cut_buffer(CUTS, blocks), cut_buffer(CUTS, blocks),
            *[half_buffer(TURNS, blocks // TURNS) for _ in range(3)],
            whole_buffer(blocks), whole_buffer(blocks),
            cut_buffer(CUTS, blocks), cut_buffer(CUTS, blocks), cut_buffer(CUTS, blocks),
            half_buffer(cross), half_buffer(cross),
            whole_buffer(cross), whole_buffer(cross),
            half_buffer(2, cross), half_buffer(2, cross),
            cut_buffer(2, CUTS, cross), cut_buffer(2, CUTS, cross),
            pltpu.VMEM((2 * bands, 2 * bands), jnp.float32),
            pltpu.VMEM((JOBS, 2, bands // 2, 2 * bands), jnp.float32),
            pltpu.VMEM((10, bands // 2, 2 * bands), jnp.float32),
            pltpu.SemaphoreType.DMA((3,)),
            pltpu.SemaphoreType.DMA((5, CHUNKS)),
            pltpu.SemaphoreType.DMA((8, CUTS)),
            pltpu.SemaphoreType.DMA((2, 4)),
            pltpu.SemaphoreType.DMA,
            pltpu.SemaphoreType.DMA((7, CUTS)),
            pltpu.SemaphoreType.DMA((2,)),
            pltpu.SemaphoreType.DMA((4, TURNS)),
            pltpu.SemaphoreType.DMA((2,)),
            pltpu.SemaphoreType.DMA((2, 2)),
            pltpu.SemaphoreType.DMA((2, 2, CUTS)),
            pltpu.SemaphoreType.DMA((2, 10)),
        ],
        compiler_params=pltpu.CompilerParams(
            collective_id=0, has_side_effects=True, vmem_limit_bytes=61 * 2**20
        ),
        name="overlaps",
    )(neighbour, shift_id, block_map, coeffs.reshape(blocks, 2 * bands, lanes))
    return found[None]


def solution(mesh):
    in_specs = (P("ka", "ga", None, None, None), P("ka", None), P("ka", None), P())
    out_specs = P("ka", None, None, "ga", None)
    return jax.shard_map(
        on_device, mesh=mesh, in_specs=in_specs, out_specs=out_specs, check_vma=False
    )
```

```python
import functools

import jax
import jax.numpy as jnp
from jax import lax
from jax.experimental import pallas as pl
from jax.experimental.pallas import tpu as pltpu
from jax.sharding import PartitionSpec as P

MESH = pl.DeviceIdType.MESH
CHUNKS = 8
CUTS = 4
TURNS = 12
LEFT_OWN, LEFT_ASIDE = (0, 1, 2), (3, 4, 5)
RIGHT_OWN, RIGHT_ASIDE = (6, 7, 8), (9, 10, 11)
LEFT = LEFT_OWN + LEFT_ASIDE
RIGHT = RIGHT_OWN + RIGHT_ASIDE
PACK = 5
STEP = 20
CONTRACT = (((1,), (1,)), ((), ()))

LOAD, ROW_SENT, RELAY_IN, RELAY_SENT, ROW_IN = range(5)
RIGHT1_SENT, RIGHT1_IN, RIGHT2_SENT, RIGHT2_IN = range(4)
LEFT1_SENT, LEFT1_IN, LEFT2_SENT, LEFT2_IN = range(4, 8)
ROW_JOB, NEXT_JOB, PREV_JOB, FAR_JOB, BACK_JOB, WRAP_JOB = range(6)
JOBS = 6


def flipped(block):
    half = block.shape[1] // 2
    return jnp.concatenate([block[:, half:], -block[:, :half]], axis=1)


def kernel(
    n_ka, row, cross, neighbour_in, shift_in, map_in, coeffs, out,
    neighbour, shift_id, block_map,    shifts_out, shifts_in, table_rows, table, own, packed, right1, right2_0, right2_1, right2_2, right2_3, left1, left2,
    extra, extra_out, extra_via, relay, ahead, near, pass_a, pass_b, wrap_out, wrap_in,
    row_out, row_in, cross_out, cross_in, far_out, far_in, row_total, parts, inbox,
    small_sem, chunk_sem, hop_sem, shift_sem, table_sem, near_sem, wrap_sem, extra_sem, row_cross_sem, cross_sem,
    far_sem, result_sem,
):
    blocks = own.shape[0]
    bands = own.shape[1] // 2
    lanes = own.shape[2]
    deep = bands // CUTS
    right2 = (right2_0, right2_1, right2_2, right2_3)
    size = blocks // CHUNKS
    inside = blocks - cross
    turn_size = blocks // TURNS
    ka = lax.axis_index("ka")
    ga = lax.axis_index("ga")
    other = 1 - ga
    core = lax.rem(ka, 2)
    place = lax.rem(ka, row)
    odd = lax.rem(place // 4, 2)
    aside = 4 - 8 * odd
    turned = jnp.where(odd == 1, 3 - 2 * core, 2 * core)
    plane = lax.rem(ka // row + turned, 8)
    beside = lax.rem(ka // row + 3 - turned, 4)
    first = place == 0
    last = place == row - 1
    quad = lax.rem(plane, 4)
    half = plane // 4
    needs_row = (core == 0) | last
    next_half = lax.rem(plane + 1, 8) // 4

    def at(step):
        return lax.rem(ka + n_ka + step, n_ka)

    def part(c):
        return pl.ds(c * size, size)

    def remote(source, target, sent, arrived, device):
        return pltpu.make_async_remote_copy(
            src_ref=source, dst_ref=target, send_sem=sent, recv_sem=arrived,
            device_id=device, device_id_type=MESH,
        )

    def load(i):
        lines = pl.ds((i // 2 + lax.rem(i, 2) * CUTS) * deep, deep)
        return pltpu.make_async_copy(
            coeffs.at[:, lines], own.at[:, lines], chunk_sem.at[LOAD, i]
        )

    def row_direct(c):
        return remote(
            own.at[part(c)], ahead.at[part(c)],
            chunk_sem.at[ROW_SENT, c], chunk_sem.at[ROW_IN, c], (at(-1), ga),
        )

    def row_relayed(c):
        return remote(
            own.at[part(c)], relay.at[part(c)],
            chunk_sem.at[ROW_SENT, c], chunk_sem.at[RELAY_IN, c], (at(-1), other),
        )

    def relayed(c):
        return remote(
            relay.at[part(c)], ahead.at[part(c)],
            chunk_sem.at[RELAY_SENT, c], chunk_sem.at[ROW_IN, c], (ka, other),
        )

    def hop(source, target, sent, cut, step):
        return remote(
            source, target, hop_sem.at[sent, cut], hop_sem.at[sent + 1, cut], (at(step * row), ga)
        )

    def hop_right(cut):
        return hop(packed.at[half, cut], right1.at[cut], RIGHT1_SENT, cut, 1)

    def hop_left(cut):
        return hop(packed.at[1 - half, cut], left1.at[cut], LEFT1_SENT, cut, -1)

    def on_right(cut):
        return hop(right1.at[cut], right2[cut], RIGHT2_SENT, cut, 1)

    def on_left(cut):
        return hop(left1.at[cut], left2.at[cut], LEFT2_SENT, cut, -1)

    def hop_extra(turn):
        return remote(
            extra_out.at[turn], extra.at[turn],
            extra_sem.at[0, turn], extra_sem.at[1, turn],
            (at(-row if turn in LEFT else row), ga),
        )

    def extra_aside(turn):
        return remote(
            extra_out.at[turn], extra_via.at[turn],
            extra_sem.at[0, turn], extra_sem.at[2, turn], (at(aside), ga),
        )

    def extra_back(turn):
        return remote(
            extra_via.at[turn], extra.at[turn],
            extra_sem.at[3, turn], extra_sem.at[1, turn],
            (at(aside + (-row if turn in LEFT else row)), ga),
        )

    def carry_left(cut):
        return remote(
            left1.at[cut], pass_a.at[cut],
            near_sem.at[0, cut], near_sem.at[1, cut], (at(row - 1), other),
        )

    def carry_right(cut):
        return remote(
            right1.at[cut], pass_b.at[cut],
            near_sem.at[2, cut], near_sem.at[3, cut], (ka, other),
        )

    def to_last(cut):
        return remote(
            pass_a.at[cut], near.at[cut], near_sem.at[4, cut], near_sem.at[5, cut], (ka, other)
        )

    def to_first(cut):
        return remote(
            pass_b.at[cut], near.at[cut],
            near_sem.at[6, cut], near_sem.at[5, cut], (at(1 - row), other),
        )

    def swap_wrap():
        return remote(wrap_out, wrap_in, wrap_sem.at[0], wrap_sem.at[1], (ka, other))

    def swap_row():
        return remote(row_out, row_in, row_cross_sem.at[0], row_cross_sem.at[1], (ka, other))

    def swap(i):
        return remote(
            cross_out.at[i], cross_in.at[i], cross_sem.at[0, i], cross_sem.at[1, i], (ka, other)
        )

    def swap_far(i, cut):
        return remote(
            far_out.at[i, cut], far_in.at[i, cut],
            far_sem.at[0, i, cut], far_sem.at[1, i, cut], (ka, other),
        )

    def result(slot):
        job, step, same = RESULTS[slot]
        side = ga if same else other
        return remote(
            parts.at[job, side], inbox.at[slot],
            result_sem.at[0, slot], result_sem.at[1, slot], (at(step), side),
        )

    RESULTS = (
        (ROW_JOB, 0, False), (NEXT_JOB, 0, False),
        (PREV_JOB, -row, True), (PREV_JOB, -row, False),
        (FAR_JOB, -2 * row, True), (FAR_JOB, -2 * row, False),
        (BACK_JOB, 2 * row, True), (BACK_JOB, 2 * row, False),
        (WRAP_JOB, -1, True), (WRAP_JOB, -1, False),
    )
    WRAPPED = (8, 9)

    def each(body):
        def run(c, carry):
            body(c)
            return carry
        lax.fori_loop(0, CHUNKS, run, 0)

    def bra_at(job, t):
        return table[job, t]

    def ket_at(job, t):
        return table[JOBS + job, t]

    def far_ket_at(job, t):
        return table[2 * JOBS + job, inside + t]

    def whole(source, index):
        return jnp.concatenate([source[cut, index] for cut in range(CUTS)], axis=0)

    def whole_far(index):
        return jnp.concatenate([right2[cut][index] for cut in range(CUTS)], axis=0)

    def gather(target, pick, count=cross):
        def run(t, carry):
            for u in range(PACK):
                target[t * PACK + u] = pick(t * PACK + u)
            return carry
        lax.fori_loop(0, count // PACK, run, 0)

    def whole_sum(total, bra, ket, count):
        def run(s, total):
            left = jnp.concatenate([bra(s * STEP + u) for u in range(STEP)], axis=1)
            right = jnp.concatenate([ket(s * STEP + u) for u in range(STEP)], axis=1)
            return total + lax.dot_general(
                left, right, CONTRACT, preferred_element_type=jnp.float32
            )
        return lax.fori_loop(0, count // STEP, run, total)

    def packed_step(total, pairs):
        left = jnp.concatenate([bra for bra, _ in pairs], axis=1)
        right = jnp.concatenate(
            [jnp.concatenate([ket for _, ket in pairs], axis=1),
             jnp.concatenate([flipped(ket) for _, ket in pairs], axis=1)], axis=0
        )
        return total + lax.dot_general(
            left, right, CONTRACT, preferred_element_type=jnp.float32
        )

    def packed_sums(totals, sources, count, width=STEP):
        def run(s, totals):
            return tuple(
                packed_step(
                    total, [(bra(s * width + u), ket(s * width + u)) for u in range(width)]
                )
                for total, (bra, ket) in zip(totals, sources)
            )
        return lax.fori_loop(0, count // width, run, tuple(totals))

    def packed_sum(total, bra, ket, count):
        return packed_sums((total,), ((bra, ket),), count)[0]

    def keep(job, total):
        parts[job] = total.reshape(parts.shape[1:])

    zero = jnp.zeros((bands, 2 * bands), jnp.float32)

    barrier = pltpu.get_barrier_semaphore()
    meet = [
        (ka, other), (at(row), ga), (at(-row), ga), (at(row), other), (at(-row), other),
        (at(2 * row), ga), (at(-2 * row), ga), (at(2 * row), other), (at(-2 * row), other),
        (at(-1), ga), (at(1), ga), (at(-1), other), (at(1), other),
        (at(aside), ga), (at(aside + row), ga), (at(aside - row), ga),
    ]
    def greet(device):
        pl.semaphore_signal(barrier, inc=1, device_id=device, device_id_type=MESH)

    for device in meet:
        greet(device)

    @pl.when(first)
    def _():
        greet((at(row - 1), other))

    @pl.when(last)
    def _():
        greet((at(1 - row), other))

    small = [
        pltpu.make_async_copy(given, held, small_sem.at[i])
        for i, (given, held) in enumerate(
            ((neighbour_in, neighbour), (shift_in, shift_id), (map_in, block_map))
        )
    ]
    for copy in small:
        copy.start()
    load(0).start()
    load(1).start()
    for copy in small:
        copy.wait()

    tile = (8, lanes)
    columns = neighbour.shape[1]
    targets = [jnp.broadcast_to(neighbour[:, b : b + 1], tile) for b in range(columns)]
    steps = (1, row, n_ka // 2)

    def shift_of(step):
        found = jnp.zeros(tile, jnp.int32)
        for b in range(columns):
            moved = jnp.broadcast_to(shift_id[:, b : b + 1], tile)
            found = found + jnp.where(targets[b] == at(step), moved, 0)
        return found

    row_shift, next_shift, far_shift = [shift_of(step) for step in steps]
    shifts_out[0] = next_shift
    shifts_out[1] = far_shift
    shifts_out[2] = row_shift

    def send_shift(i):
        return remote(
            shifts_out.at[(0, 1, 1, 2)[i]], shifts_in.at[i],
            shift_sem.at[0, i], shift_sem.at[1, i], (at((row, 2 * row, -2 * row, 1)[i]), ga),
        )

    def load_cut(cut):
        load(2 * cut).wait()
        load(2 * cut + 1).wait()

    def pack_cut(cut):
        def pack(t, carry):
            for u in range(STEP):
                j = t * STEP + u
                real = own[j, pl.ds(cut * deep, deep), :]
                imag = own[j, pl.ds(bands + cut * deep, deep), :]
                mid = lanes // 2
                packed[0, cut, j] = jnp.concatenate([real[:, :mid], imag[:, :mid]], axis=1)
                packed[1, cut, j] = jnp.concatenate([real[:, mid:], imag[:, mid:]], axis=1)
            return carry
        lax.fori_loop(0, blocks // STEP, pack, 0)

    load_cut(0)
    for i in range(2, CHUNKS):
        load(i).start()
    pack_cut(0)
    pl.semaphore_wait(barrier, len(meet) + jnp.where(first | last, 1, 0))
    for i in range(4):
        send_shift(i).start()

    def make_table():
        lane = lax.broadcasted_iota(jnp.int32, (lanes, lanes), 1)
        line = lax.broadcasted_iota(jnp.int32, (lanes, lanes), 0)
        maps = [
            jnp.concatenate(
                [block_map[:, a * blocks : (a + 1) * blocks],
                 jnp.zeros((block_map.shape[0], lanes - blocks), jnp.int32)], axis=1
            )
            for a in range(2)
        ]
        maps = [jnp.where(ga == a, maps[0], maps[1]) for a in range(2)]
        shifts = [row_shift, next_shift] + [shifts_in[i] for i in range(4)]
        choice = lax.broadcasted_iota(jnp.int32, tile, 0)
        rows = [
            jnp.sum(jnp.where(shift == choice, each_map, 0), axis=0, keepdims=True)
            for each_map in maps for shift in shifts
        ]
        rows = jnp.concatenate(rows + [jnp.zeros((16 - 2 * JOBS, lanes), jnp.int32)], axis=0)
        number = lax.broadcasted_iota(jnp.int32, rows.shape, 0)
        spot = lax.broadcasted_iota(jnp.int32, rows.shape, 1)
        source = jnp.where(rows >= blocks, 1, 0)
        same = jnp.where(source == jnp.where(number < JOBS, ga, other), 1, 0)
        local = rows - blocks * source
        same_t = same.T
        kept = [
            jnp.sum(jnp.where(line < lane, same_t[:, r : r + 1], 0), axis=0, keepdims=True)
            for r in range(2 * JOBS)
        ]
        kept = jnp.concatenate(kept + [jnp.zeros((16 - 2 * JOBS, lanes), jnp.int32)], axis=0)
        rank = jnp.where(same == 1, kept, inside + spot - kept)
        rank_t = jnp.where(spot < blocks, rank, -1).T
        local_t = local.T
        hits = [rank_t[:, r : r + 1] == lane for r in range(2 * JOBS)]
        lists = [jnp.sum(jnp.where(hits[r], line, 0), axis=0, keepdims=True) for r in range(JOBS)]
        lists += [
            jnp.sum(jnp.where(hits[r], local_t[:, r : r + 1], 0), axis=0, keepdims=True)
            for r in range(2 * JOBS)
        ]
        lists += [jnp.zeros((24 - 3 * JOBS, lanes), jnp.int32)]
        table_rows[...] = jnp.concatenate(lists, axis=0)

    def first_sends(c):
        @pl.when(core == 1)
        def _():
            row_direct(c).start()

        @pl.when((core == 0) & (place > 0))
        def _():
            row_relayed(c).start()

    hop_right(0).start()
    hop_left(0).start()
    for cut in range(1, CUTS):
        load_cut(cut)
    each(first_sends)
    pack_cut(1)
    for cut in range(1, CUTS):
        if cut + 1 < CUTS:
            pack_cut(cut + 1)
        hop_right(cut).start()
        hop_left(cut).start()
    for i in range(4):
        send_shift(i).wait_recv()
    make_table()
    fetch = pltpu.make_async_copy(table_rows, table, table_sem)
    fetch.start()
    fetch.wait()
    gather(cross_out.at[0], lambda t: whole(packed.at[1 - next_half], bra_at(NEXT_JOB, inside + t)))
    gather(cross_out.at[1], lambda t: whole(packed.at[half], far_ket_at(PREV_JOB, t)))

    @pl.when(core == 0)
    def _():
        gather(row_out, lambda t: own[bra_at(ROW_JOB, inside + t)])

    @pl.when(last)
    def _():
        gather(
            row_out,
            lambda t: jnp.concatenate(
                [whole(packed.at[h], bra_at(ROW_JOB, inside + t)) for h in range(2)], axis=0
            ),
        )

    @pl.when(needs_row)
    def _():
        swap_row().start()

    @pl.when(first)
    def _():
        gather(wrap_out, lambda t: whole(packed.at[half], far_ket_at(WRAP_JOB, t)))
        swap_wrap().start()

    swap(0).start()
    swap(1).start()

    @pl.when(quad == 3)
    def _():
        for turn in RIGHT_ASIDE + RIGHT_OWN:
            gather(
                extra_out.at[turn],
                lambda t: whole(packed.at[1 - half], bra_at(NEXT_JOB, turn * turn_size + t)),
                turn_size,
            )
        for turn in RIGHT_ASIDE:
            extra_aside(turn).start()

    @pl.when(quad == 0)
    def _():
        for turn in LEFT_ASIDE + LEFT_OWN:
            gather(
                extra_out.at[turn],
                lambda t: whole(packed.at[half], ket_at(PREV_JOB, turn * turn_size + t)),
                turn_size,
            )
        for turn in LEFT_ASIDE:
            extra_aside(turn).start()

    def pass_near(cut):
        carry_left(cut).wait_recv()
        to_last(cut).start()
        carry_right(cut).wait_recv()
        to_first(cut).start()

    def relay_on(c):
        row_relayed(c).wait_recv()
        relayed(c).start()

    for cut in range(CUTS):
        hop_right(cut).wait_recv()
        on_right(cut).start()
        hop_left(cut).wait_recv()

        on_left(cut).start()

        @pl.when(first)
        def _(cut=cut):
            carry_left(cut).start()

        @pl.when(last)
        def _(cut=cut):
            carry_right(cut).start()
            if cut:
                pass_near(cut - 1)

        @pl.when((core == 1) & (place < row - 1))
        def _(cut=cut):
            for c in range(cut * CHUNKS // CUTS, (cut + 1) * CHUNKS // CUTS):
                relay_on(c)

    @pl.when(quad == 3)
    def _():
        for turn in RIGHT_OWN:
            hop_extra(turn).start()

    @pl.when(quad == 0)
    def _():
        for turn in LEFT_OWN:
            hop_extra(turn).start()

    @pl.when(beside == 3)
    def _():
        for turn in RIGHT_ASIDE:
            extra_aside(turn).wait_recv()
            extra_back(turn).start()

    @pl.when(beside == 0)
    def _():
        for turn in LEFT_ASIDE:
            extra_aside(turn).wait_recv()
            extra_back(turn).start()

    @pl.when(last)
    def _():
        pass_near(CUTS - 1)

    swap(0).wait_recv()
    total = packed_sum(
        zero,
        lambda t: whole(packed.at[1 - next_half], bra_at(NEXT_JOB, t)),
        lambda t: whole(left1, ket_at(NEXT_JOB, t)),
        inside,
    )
    total = packed_sum(
        total, lambda t: cross_in[0, t], lambda t: whole(left1, far_ket_at(NEXT_JOB, t)), cross
    )
    keep(NEXT_JOB, total)

    swap(1).wait_recv()

    @pl.when(quad != 0)
    def _():
        total = packed_sum(
            zero,
            lambda t: whole(right1, bra_at(PREV_JOB, t)),
            lambda t: whole(packed.at[half], ket_at(PREV_JOB, t)),
            inside,
        )
        total = packed_sum(
            total,
            lambda t: whole(right1, bra_at(PREV_JOB, inside + t)),
            lambda t: cross_in[1, t],
            cross,
        )
        keep(PREV_JOB, total)

    @pl.when(quad != 3)
    def _():
        result(1).start()

    def along_row():
        each(lambda c: row_direct(c).wait_recv())
        row_total[...] = whole_sum(
            jnp.zeros(row_total.shape, jnp.float32),
            lambda t: own[bra_at(ROW_JOB, t)],
            lambda t: ahead[ket_at(ROW_JOB, t)],
            inside,
        )

        @pl.when(core == 0)
        def _():
            swap_row().wait_recv()
            row_total[...] = whole_sum(
                row_total[...], lambda t: row_in[t], lambda t: ahead[far_ket_at(ROW_JOB, t)], cross
            )

        @pl.when(core == 1)
        def _():
            row_total[...] = whole_sum(
                row_total[...],
                lambda t: own[bra_at(ROW_JOB, inside + t)],
                lambda t: relay[ket_at(ROW_JOB, inside + t)],
                cross,
            )

        lower = row_total[pl.ds(bands, bands)]
        keep(
            ROW_JOB,
            row_total[pl.ds(0, bands)]
            + jnp.concatenate([lower[:, bands:], -lower[:, :bands]], axis=1),
        )
        result(0).start()

    @pl.when(core == 0)
    def _():
        along_row()

    def wrap_at_last():
        for cut in range(CUTS):
            to_last(cut).wait_recv()
        swap_row().wait_recv()
        lines = pl.ds(pl.multiple_of((1 - half) * bands, bands), bands)
        total = packed_sum(
            zero,
            lambda t: whole(packed.at[1 - half], bra_at(ROW_JOB, t)),
            lambda t: whole(near, ket_at(ROW_JOB, t)),
            inside,
        )
        total = packed_sum(
            total,
            lambda t: row_in[t, lines, :],
            lambda t: whole(near, far_ket_at(ROW_JOB, t)),
            cross,
        )
        keep(ROW_JOB, total)
        result(0).start()

    def wrap_at_first():
        for cut in range(CUTS):
            to_last(cut).wait_recv()
        swap_wrap().wait_recv()
        total = packed_sum(
            zero,
            lambda t: whole(near, bra_at(WRAP_JOB, t)),
            lambda t: whole(packed.at[half], ket_at(WRAP_JOB, t)),
            inside,
        )
        total = packed_sum(
            total,
            lambda t: whole(near, bra_at(WRAP_JOB, inside + t)),
            lambda t: wrap_in[t],
            cross,
        )
        keep(WRAP_JOB, total)
        for slot in WRAPPED:
            result(slot).start()

    def far_swaps(cut):
        on_right(cut).wait_recv()
        gather(far_out.at[0, cut], lambda t: right2[cut][bra_at(FAR_JOB, inside + t)])
        gather(far_out.at[1, cut], lambda t: right2[cut][far_ket_at(BACK_JOB, t)])
        swap_far(0, cut).start()
        swap_far(1, cut).start()

    far_swaps(0)

    @pl.when(quad != 0)
    def _():
        result(2).start()
        result(3).start()

    for cut in range(1, CUTS):
        if cut == CUTS - 1:
            @pl.when((core == 1) & (place < row - 1))
            def _():
                along_row()

            @pl.when(last)
            def _():
                wrap_at_last()

            @pl.when(first)
            def _():
                wrap_at_first()

        far_swaps(cut)

    def previous_extra(turn):
        if turn * turn_size < inside:
            ket = lambda t: whole(packed.at[half], ket_at(PREV_JOB, turn * turn_size + t))
        else:
            ket = lambda t: cross_in[1, turn * turn_size - inside + t]
        return lambda t: extra[turn, t], ket

    def next_extra(turn):
        return (
            lambda t: whole(packed.at[1 - half], bra_at(NEXT_JOB, turn * turn_size + t)),
            lambda t: extra[turn, t],
        )

    def extra_sum(turns, source):
        totals = (zero, zero)
        for pair in turns:
            for turn in pair:
                hop_extra(turn).wait_recv()
            totals = packed_sums(totals, [source(turn) for turn in pair], turn_size, turn_size)
        return totals[0] + totals[1]

    def kept(job):
        return parts[job].reshape(zero.shape)

    from_left = tuple(zip(RIGHT_OWN, RIGHT_ASIDE))
    from_right = tuple(zip(LEFT_OWN, LEFT_ASIDE))

    for cut in range(CUTS):
        on_left(cut).wait_recv()
    far, back = packed_sums(
        (zero, zero),
        (
            (lambda t: whole_far(bra_at(FAR_JOB, t)), lambda t: whole(left2, ket_at(FAR_JOB, t))),
            (lambda t: whole(left2, bra_at(BACK_JOB, t)), lambda t: whole_far(ket_at(BACK_JOB, t))),
        ),
        inside,
    )

    @pl.when(quad == 0)
    def _():
        keep(PREV_JOB, extra_sum(from_left[:2], previous_extra))

    @pl.when(quad == 3)
    def _():
        keep(NEXT_JOB, kept(NEXT_JOB) + extra_sum(from_right[:2], next_extra))

    for cut in range(CUTS):
        swap_far(0, cut).wait_recv()
        swap_far(1, cut).wait_recv()
    far, back = packed_sums(
        (far, back),
        (
            (
                lambda t: whole(far_in.at[0], t),
                lambda t: whole(left2, far_ket_at(FAR_JOB, t)),
            ),
            (
                lambda t: whole(left2, bra_at(BACK_JOB, inside + t)),
                lambda t: whole(far_in.at[1], t),
            ),
        ),
        cross,
    )
    keep(FAR_JOB, far)
    keep(BACK_JOB, back)
    for slot in (4, 5, 6, 7):
        result(slot).start()

    @pl.when(quad == 0)
    def _():
        keep(PREV_JOB, kept(PREV_JOB) + extra_sum(from_left[2:], previous_extra))
        result(2).start()
        result(3).start()

    @pl.when(quad == 3)
    def _():
        keep(NEXT_JOB, kept(NEXT_JOB) + extra_sum(from_right[2:], next_extra))
        result(1).start()

    def drain(c):
        @pl.when(place > 0)
        def _():
            row_direct(c).wait_send()

        @pl.when((core == 1) & (place < row - 1))
        def _():
            relayed(c).wait_send()

    each(drain)
    for cut in range(CUTS):
        hop_right(cut).wait_send()
        hop_left(cut).wait_send()
        on_right(cut).wait_send()
        on_left(cut).wait_send()
        swap_far(0, cut).wait_send()
        swap_far(1, cut).wait_send()
    for i in range(4):
        send_shift(i).wait_send()

    @pl.when(quad == 3)
    def _():
        for turn in RIGHT:
            hop_extra(turn).wait_send()

    @pl.when(quad == 0)
    def _():
        for turn in LEFT:
            hop_extra(turn).wait_send()

    @pl.when(beside == 3)
    def _():
        for turn in RIGHT_ASIDE:
            extra_back(turn).wait_send()

    @pl.when(beside == 0)
    def _():
        for turn in LEFT_ASIDE:
            extra_back(turn).wait_send()

    @pl.when(first)
    def _():
        swap_wrap().wait_send()
        for cut in range(CUTS):
            carry_left(cut).wait_send()

    @pl.when(last)
    def _():
        for cut in range(CUTS):
            carry_right(cut).wait_send()
            to_last(cut).wait_send()
            to_first(cut).wait_send()

    @pl.when(needs_row)
    def _():
        swap_row().wait_send()

    for i in range(2):
        swap(i).wait_send()
    for slot in range(WRAPPED[0]):
        result(slot).wait_recv()
    inbox[0] = inbox[0] + parts[ROW_JOB, ga]

    @pl.when(last)
    def _():
        for slot in WRAPPED:
            result(slot).wait_recv()
        inbox[0] = inbox[0] + (inbox[8] + inbox[9])

    found = [
        inbox[0],
        (parts[NEXT_JOB, ga] + inbox[1]) + (inbox[2] + inbox[3]),
        (inbox[4] + inbox[5]) + (inbox[6] + inbox[7]),
    ]
    for b in range(columns):
        target = jnp.broadcast_to(neighbour[:, b : b + 1], found[0].shape)
        chosen = jnp.where(
            target == at(steps[0]), found[0], jnp.where(target == at(steps[1]), found[1], found[2])
        )
        out[b, 0] = chosen[:, :bands]
        out[b, 1] = chosen[:, bands:]

    for slot in range(WRAPPED[0]):
        result(slot).wait_send()

    @pl.when(first)
    def _():
        for slot in WRAPPED:
            result(slot).wait_send()


def on_device(coeffs, neighbour, shift_id, block_map):
    _, blocks, _, bands, lanes = coeffs.shape
    columns = neighbour.shape[1]
    n_ka = lax.axis_size("ka")
    row = n_ka // 8
    cross = 2 * max(1, blocks // 12)
    def half_buffer(*lead):
        return pltpu.VMEM((*lead, bands, lanes), jnp.bfloat16)

    def cut_buffer(*lead):
        return pltpu.VMEM((*lead, bands // CUTS, lanes), jnp.bfloat16)

    def whole_buffer(*lead):
        return pltpu.VMEM((*lead, 2 * bands, lanes), jnp.bfloat16)

    found = pl.pallas_call(
        functools.partial(kernel, n_ka, row, cross),
        out_shape=pltpu.VMEM((columns, 2, bands // 2, bands), jnp.float32),
        in_specs=[
            pl.BlockSpec(memory_space=pl.ANY),
            pl.BlockSpec(memory_space=pl.ANY),
            pl.BlockSpec(memory_space=pl.ANY),
            pl.BlockSpec(memory_space=pl.ANY),
        ],
        out_specs=pl.BlockSpec(memory_space=pltpu.VMEM),
        scratch_shapes=[
            pltpu.VMEM(neighbour.shape, jnp.int32),
            pltpu.VMEM(shift_id.shape, jnp.int32),
            pltpu.VMEM(block_map.shape, jnp.int32),
            pltpu.VMEM((3, 8, lanes), jnp.int32),
            pltpu.VMEM((4, 8, lanes), jnp.int32),
            pltpu.VMEM((24, lanes), jnp.int32),
            pltpu.SMEM((24, lanes), jnp.int32),
            whole_buffer(blocks),
            cut_buffer(2, CUTS, blocks),
            cut_buffer(CUTS, blocks),
            *[cut_buffer(blocks) for _ in range(CUTS)],
            cut_buffer(CUTS, blocks), cut_buffer(CUTS, blocks),
            *[half_buffer(TURNS, blocks // TURNS) for _ in range(3)],
            whole_buffer(blocks), whole_buffer(blocks),
            cut_buffer(CUTS, blocks), cut_buffer(CUTS, blocks), cut_buffer(CUTS, blocks),
            half_buffer(cross), half_buffer(cross),
            whole_buffer(cross), whole_buffer(cross),
            half_buffer(2, cross), half_buffer(2, cross),
            cut_buffer(2, CUTS, cross), cut_buffer(2, CUTS, cross),
            pltpu.VMEM((2 * bands, 2 * bands), jnp.float32),
            pltpu.VMEM((JOBS, 2, bands // 2, 2 * bands), jnp.float32),
            pltpu.VMEM((10, bands // 2, 2 * bands), jnp.float32),
            pltpu.SemaphoreType.DMA((3,)),
            pltpu.SemaphoreType.DMA((5, CHUNKS)),
            pltpu.SemaphoreType.DMA((8, CUTS)),
            pltpu.SemaphoreType.DMA((2, 4)),
            pltpu.SemaphoreType.DMA,
            pltpu.SemaphoreType.DMA((7, CUTS)),
            pltpu.SemaphoreType.DMA((2,)),
            pltpu.SemaphoreType.DMA((4, TURNS)),
            pltpu.SemaphoreType.DMA((2,)),
            pltpu.SemaphoreType.DMA((2, 2)),
            pltpu.SemaphoreType.DMA((2, 2, CUTS)),
            pltpu.SemaphoreType.DMA((2, 10)),
        ],
        compiler_params=pltpu.CompilerParams(
            collective_id=0, has_side_effects=True, vmem_limit_bytes=61 * 2**20
        ),
        name="overlaps",
    )(neighbour, shift_id, block_map, coeffs.reshape(blocks, 2 * bands, lanes))
    return found[None]


def solution(mesh):
    in_specs = (P("ka", "ga", None, None, None), P("ka", None), P("ka", None), P())
    out_specs = P("ka", None, None, "ga", None)
    return jax.shard_map(
        on_device, mesh=mesh, in_specs=in_specs, out_specs=out_specs, check_vma=False
    )
```
